32 devices in a mesh: rep: 2 (over x), fsdp: 4 (over z), ns: 4 (over y, core).
Axes of the slice: x: 2, y: 2, z: 4, core: 2. Of those that a mesh axis runs over, the one named last changes fastest.
Arguments:
- tokens: bfloat16 [8192, 2048], P(('rep', 'fsdp', 'ns')), may hold values from -6 to 6
- cotangent: bfloat16 [8192, 2048], P(('rep', 'fsdp', 'ns')), may hold values from -6 to 6
- placement: int32 [8192], P(('rep', 'fsdp', 'ns')), may hold values from 0 to 8191, as said below
- lengths: int32 [2, 4], P('rep'), may hold values from 1 to 2048, 4096 in all within a row
- step_count: int32 [1], replicated, may hold values from 1 to 16
- norm_gain: float32 [2048], replicated, may hold values from 0.5 to 1.5
- norm_bias: float32 [2048], replicated, may hold values from -1.25 to 1.25
- project_weight: float32 [2048, 6144], P('fsdp', 'ns'), may hold values from -0.125 to 0.125
- project_bias: float32 [6144], P('ns'), may hold values from -1.25 to 1.25
- output_weight: float32 [2048, 2048], P('ns', 'fsdp'), may hold values from -1.5 to 1.5
- output_bias: float32 [2048], replicated, may hold values from -1.25 to 1.25
- expand_weight: float32 [2048, 8192], P('fsdp', 'ns'), may hold values from -0.125 to 0.125
- expand_bias: float32 [8192], P('ns'), may hold values from -1.25 to 1.25
- reduce_weight: float32 [8192, 2048], P('ns', 'fsdp'), may hold values from -0.0625 to 0.0625
- reduce_bias: float32 [2048], replicated, may hold values from -1.25 to 1.25
- project_momentum: float32 [2048, 6144], P('fsdp', 'ns'), may hold values from -512 to 512
- output_momentum: float32 [2048, 2048], P('ns', 'fsdp'), may hold values from -28 to 28
- expand_momentum: float32 [2048, 8192], P('fsdp', 'ns'), may hold values from -160 to 160
- reduce_momentum: float32 [8192, 2048], P('ns', 'fsdp'), may hold values from -256 to 256
- norm_gain_first: float32 [2048], replicated, may hold values from -64 to 64
- norm_gain_second: float32 [2048], replicated, may hold values from 409.6 to 1638.4
- norm_bias_first: float32 [2048], replicated, may hold values from -64 to 64
- norm_bias_second: float32 [2048], replicated, may hold values from 409.6 to 1638.4
- project_bias_first: float32 [6144], P('ns'), may hold values from -64 to 64
- project_bias_second: float32 [6144], P('ns'), may hold values from 409.6 to 1638.4
- output_bias_first: float32 [2048], replicated, may hold values from -64 to 64
- output_bias_second: float32 [2048], replicated, may hold values from 409.6 to 1638.4
- expand_bias_first: float32 [8192], P('ns'), may hold values from -64 to 64
- expand_bias_second: float32 [8192], P('ns'), may hold values from 409.6 to 1638.4
- reduce_bias_first: float32 [2048], replicated, may hold values from -64 to 64
- reduce_bias_second: float32 [2048], replicated, may hold values from 409.6 to 1638.4
Outputs:
- layer_output: bfloat16 [8192, 2048], P(('rep', 'fsdp', 'ns'))
- input_grad: bfloat16 [8192, 2048], P(('rep', 'fsdp', 'ns'))
- norm_gain_grad: float32 [2048], replicated
- norm_bias_grad: float32 [2048], replicated
- project_weight_grad: float32 [2048, 6144], P('fsdp', 'ns')
- project_bias_grad: float32 [6144], P('ns')
- output_weight_grad: float32 [2048, 2048], P('ns', 'fsdp')
- output_bias_grad: float32 [2048], replicated
- expand_weight_grad: float32 [2048, 8192], P('fsdp', 'ns')
- expand_bias_grad: float32 [8192], P('ns')
- reduce_weight_grad: float32 [8192, 2048], P('ns', 'fsdp')
- reduce_bias_grad: float32 [2048], replicated
- norm_gain_new: float32 [2048], replicated
- norm_bias_new: float32 [2048], replicated
- project_weight_new: float32 [2048, 6144], P('fsdp', 'ns')
- project_bias_new: float32 [6144], P('ns')
- output_weight_new: float32 [2048, 2048], P('ns', 'fsdp')
- output_bias_new: float32 [2048], replicated
- expand_weight_new: float32 [2048, 8192], P('fsdp', 'ns')
- expand_bias_new: float32 [8192], P('ns')
- reduce_weight_new: float32 [8192, 2048], P('ns', 'fsdp')
- reduce_bias_new: float32 [2048], replicated
- project_weight_copy: bfloat16 [2048, 6144], P('fsdp', 'ns')
- output_weight_copy: bfloat16 [2048, 2048], P('ns', 'fsdp')
- expand_weight_copy: bfloat16 [2048, 8192], P('fsdp', 'ns')
- reduce_weight_copy: bfloat16 [8192, 2048], P('ns', 'fsdp')
- project_momentum_new: float32 [2048, 6144], P('fsdp', 'ns')
- output_momentum_new: float32 [2048, 2048], P('ns', 'fsdp')
- expand_momentum_new: float32 [2048, 8192], P('fsdp', 'ns')
- reduce_momentum_new: float32 [8192, 2048], P('ns', 'fsdp')
- norm_gain_first_new: float32 [2048], replicated
- norm_gain_second_new: float32 [2048], replicated
- norm_bias_first_new: float32 [2048], replicated
- norm_bias_second_new: float32 [2048], replicated
- project_bias_first_new: float32 [6144], P('ns')
- project_bias_second_new: float32 [6144], P('ns')
- output_bias_first_new: float32 [2048], replicated
- output_bias_second_new: float32 [2048], replicated
- expand_bias_first_new: float32 [8192], P('ns')
- expand_bias_second_new: float32 [8192], P('ns')
- reduce_bias_first_new: float32 [2048], replicated
- reduce_bias_second_new: float32 [2048], replicated
The draws below stay inside these ranges and needn't reach their ends.
Inputs may be any that keep to these rules, and one draw needn't show every extreme that they name: placement is a permutation; it maps the 256 given rows of each device to packed rows of the devices with the same rep and ns index, exactly 64 to each fsdp index, into that device's block of 64 rows that starts at 64 times the sender's fsdp index. Each row of lengths sums to 4096; in each row the largest length is exactly 2048.
All inputs are finite; a program needn't handle non-finite values.
Results may differ from the reference program's by a relative error of at most 0.006.
The reference program's roundings to bfloat16 on the way count: a program that leaves them out, or rounds other values in their place, can miss the bound.
Values may be sent and summed in bfloat16 or wider, within the bound.
A program may use at most 384 MiB of HBM per device.

```python
import math
import jax
import jax.numpy as jnp
import numpy as np
from jax import lax

D = 2048
HEADS = 32
HEAD_DIM = 64
ROT = 32
FF = 8192
TS = 256
SCHULZ_STEPS = 5
PACK = 4096
TOKENS = 8192
LONGEST = 2048
SEQS = 4
SLOT = 64
N_REP = 2
N_FSDP = 4
N_NS = 4


def draw_placement(key, part):
    blocks = N_REP * N_FSDP * N_NS
    scores = jax.random.randint(key, (blocks, TS), 0, 1 << 20)
    distinct = scores * TS + jnp.arange(TS, dtype=jnp.int32)[None, :]
    ordering = jnp.argsort(distinct, axis=1).astype(jnp.int32)
    block_ids = jnp.arange(blocks, dtype=jnp.int32)
    rep_at = block_ids // (N_FSDP * N_NS)
    fsdp_at = block_ids // N_NS % N_FSDP
    ns_at = block_ids % N_NS
    slot_ids = jnp.arange(TS, dtype=jnp.int32)
    dest_fsdp = slot_ids // SLOT
    within = slot_ids % SLOT
    target = ((rep_at[:, None] * N_FSDP + dest_fsdp[None, :]) * N_NS + ns_at[:, None]) * TS + fsdp_at[:, None] * SLOT + within[None, :]
    row_ids = block_ids[:, None] * TS + ordering
    return jnp.zeros((blocks * TS,), jnp.int32).at[row_ids.reshape(-1)].set(target.reshape(-1).astype(jnp.int32))


def shard_levels(rng, dims, cuts, low, largest):
    gain = 1.0
    for axis_at, shards_of in cuts:
        heights = jax.random.uniform(jax.random.fold_in(jax.random.fold_in(rng, 6), axis_at), (shards_of,), jnp.float32, low / len(cuts), largest / len(cuts))
        gain = gain * jnp.repeat(jnp.exp(heights), dims[axis_at] // shards_of).reshape((-1,) + (1,) * (len(dims) - 1 - axis_at))
    return gain


def length_profile(number_of, total, most, skew):
    weights = [(1 << 20) // math.isqrt(rank ** skew) + 1 for rank in range(2, number_of + 1)]
    surplus, counts = total - most - (number_of - 1), [1] * (number_of - 1)
    while surplus > 0:
        free = [i for i in range(number_of - 1) if counts[i] < most]
        mass, left = sum([weights[i] for i in free]), surplus
        for i in free:
            addition = min(most - counts[i], max(1, left * weights[i] // mass), surplus)
            counts[i] = counts[i] + addition
            surplus = surplus - addition
    return np.array([most] + counts)


def uneven_parts(rng, number_of, total, most, lean):
    if number_of == 2:
        one = jax.random.randint(rng, (), max(1, total - most), min(most, total - 1) + 1)
        return jnp.stack([one, total - one])
    tallies = jnp.asarray(length_profile(number_of, total, most, lean), jnp.int32)
    couples = (number_of - 1) // 2
    giver, receiver = tallies[1:1 + 2 * couples:2], tallies[2:2 + 2 * couples:2]
    margin = jnp.minimum(giver - 1, most - receiver)
    passed = jax.random.randint(jax.random.fold_in(rng, 1), (couples,), 0, 1 << 20) % (margin + 1)
    tallies = tallies.at[1:1 + 2 * couples:2].set(giver - passed).at[2:2 + 2 * couples:2].set(receiver + passed)
    return tallies[jax.random.permutation(jax.random.fold_in(rng, 2), number_of)]


def bell_draw(own_key, dims, scale, limit, split=(), kind=jnp.bfloat16):
    gain = shard_levels(own_key, dims, split, -0.22, 0.18) if split else 1.0
    values = jax.random.normal(own_key, dims, jnp.float32) * scale * gain
    return jnp.minimum(jnp.maximum(values, -limit), limit).astype(kind)


def setup_inputs(seed: int = 0) -> dict:
    arg_keys = jax.random.split(jax.random.key(seed), 32)
    tokens = bell_draw(arg_keys[0], (TOKENS, D), 1.0, 6.0, ((0, 32),))
    cotangent = bell_draw(arg_keys[1], (TOKENS, D), 1.0, 6.0, ((0, 32),))
    placement = draw_placement(jax.random.fold_in(arg_keys[31], 71), 0)
    lengths = jax.vmap(lambda own: uneven_parts(own, SEQS, PACK, LONGEST, 2))(jax.random.split(arg_keys[3], N_REP)).reshape((N_REP, SEQS)).astype(jnp.int32)
    step_count = jax.random.randint(arg_keys[4], (1,), 1, 17).astype(jnp.int32)
    norm_gain = jnp.clip(1.0 + 0.1 * jax.random.normal(arg_keys[5], (D,), jnp.float32), 0.5, 1.5)
    norm_bias = bell_draw(arg_keys[6], (D,), 0.2, 1.25, (), jnp.float32)
    project_weight = bell_draw(arg_keys[7], (D, 3 * D), D ** -0.5, 0.125, ((0, 4), (1, 4)), jnp.float32)
    project_bias = bell_draw(arg_keys[8], (3 * D,), 0.2, 1.25, ((0, 4),), jnp.float32)
    output_weight = bell_draw(arg_keys[9], (D, D), (D // 128) ** -0.5, 1.5, ((0, 4), (1, 4)), jnp.float32)
    output_bias = bell_draw(arg_keys[10], (D,), 0.2, 1.25, (), jnp.float32)
    expand_weight = bell_draw(arg_keys[11], (D, FF), D ** -0.5, 0.125, ((0, 4), (1, 4)), jnp.float32)
    expand_bias = bell_draw(arg_keys[12], (FF,), 0.2, 1.25, ((0, 4),), jnp.float32)
    reduce_weight = bell_draw(arg_keys[13], (FF, D), FF ** -0.5, 0.0625, ((0, 4), (1, 4)), jnp.float32)
    reduce_bias = bell_draw(arg_keys[14], (D,), 0.2, 1.25, (), jnp.float32)
    project_momentum = bell_draw(arg_keys[15], (D, 3 * D), (1.0 * TOKENS ** 0.5), 512.0, ((0, 4), (1, 4)), jnp.float32)
    output_momentum = bell_draw(arg_keys[16], (D, D), (0.05 * TOKENS ** 0.5), 28.0, ((0, 4), (1, 4)), jnp.float32)
    expand_momentum = bell_draw(arg_keys[17], (D, FF), (0.3 * TOKENS ** 0.5), 160.0, ((0, 4), (1, 4)), jnp.float32)
    reduce_momentum = bell_draw(arg_keys[18], (FF, D), (0.5 * TOKENS ** 0.5), 256.0, ((0, 4), (1, 4)), jnp.float32)
    norm_gain_first = bell_draw(arg_keys[19], (D,), (0.11 * TOKENS ** 0.5), 64.0, (), jnp.float32)
    norm_gain_second = jnp.clip(jax.random.uniform(arg_keys[20], (D,), jnp.float32, 409.6, 1638.4), 409.6, 1638.4)
    norm_bias_first = bell_draw(arg_keys[21], (D,), (0.11 * TOKENS ** 0.5), 64.0, (), jnp.float32)
    norm_bias_second = jnp.clip(jax.random.uniform(arg_keys[22], (D,), jnp.float32, 409.6, 1638.4), 409.6, 1638.4)
    project_bias_first = bell_draw(arg_keys[23], (3 * D,), (0.11 * TOKENS ** 0.5), 64.0, ((0, 4),), jnp.float32)
    project_bias_second = jnp.clip(409.6 + 1228.8 * jax.random.uniform(arg_keys[24], (3 * D,), jnp.float32) ** shard_levels(arg_keys[24], (3 * D,), ((0, 4),), -0.2, 0.2), 409.6, 1638.4)
    output_bias_first = bell_draw(arg_keys[25], (D,), (0.11 * TOKENS ** 0.5), 64.0, (), jnp.float32)
    output_bias_second = jnp.clip(jax.random.uniform(arg_keys[26], (D,), jnp.float32, 409.6, 1638.4), 409.6, 1638.4)
    expand_bias_first = bell_draw(arg_keys[27], (FF,), (0.11 * TOKENS ** 0.5), 64.0, ((0, 4),), jnp.float32)
    expand_bias_second = jnp.clip(409.6 + 1228.8 * jax.random.uniform(arg_keys[28], (FF,), jnp.float32) ** shard_levels(arg_keys[28], (FF,), ((0, 4),), -0.2, 0.2), 409.6, 1638.4)
    reduce_bias_first = bell_draw(arg_keys[29], (D,), (0.11 * TOKENS ** 0.5), 64.0, (), jnp.float32)
    reduce_bias_second = jnp.clip(jax.random.uniform(arg_keys[30], (D,), jnp.float32, 409.6, 1638.4), 409.6, 1638.4)
    return dict(tokens=tokens, cotangent=cotangent, placement=placement, lengths=lengths, step_count=step_count, norm_gain=norm_gain, norm_bias=norm_bias, project_weight=project_weight, project_bias=project_bias, output_weight=output_weight, output_bias=output_bias, expand_weight=expand_weight, expand_bias=expand_bias, reduce_weight=reduce_weight, reduce_bias=reduce_bias, project_momentum=project_momentum, output_momentum=output_momentum, expand_momentum=expand_momentum, reduce_momentum=reduce_momentum, norm_gain_first=norm_gain_first, norm_gain_second=norm_gain_second, norm_bias_first=norm_bias_first, norm_bias_second=norm_bias_second, project_bias_first=project_bias_first, project_bias_second=project_bias_second, output_bias_first=output_bias_first, output_bias_second=output_bias_second, expand_bias_first=expand_bias_first, expand_bias_second=expand_bias_second, reduce_bias_first=reduce_bias_first, reduce_bias_second=reduce_bias_second)


@jax.custom_vjp
def low(v):
    return lax.optimization_barrier(v.astype(jnp.bfloat16)).astype(jnp.float32)

@jax.custom_vjp
def low_back(v):
    return v

def low_keep(v):
    return (low(v), None)

def low_pass(kept, grad):
    return (grad,)

def back_keep(v):
    return (v, None)

def back_low(kept, grad):
    return (low(grad),)
low.defvjp(low_keep, low_pass)
low_back.defvjp(back_keep, back_low)
PRECISE = lax.Precision.HIGHEST
NORM_EPSILON = 1e-05
ROPE_BASE = 10000.0
NEG_LARGE = -1e+30
SCHULZ_FIRST = 3.4445
SCHULZ_SECOND = -4.775
SCHULZ_THIRD = 2.0315
SCHULZ_EPSILON = 1e-06
MUON_RATE = 0.2
MUON_DECAY = 0.5
RMS_MATCH = 0.2
WEIGHT_DECAY = 0.1
ADAM_RATE = 0.2
ADAM_FIRST = 0.9
ADAM_SECOND = 0.95
ADAM_EPSILON = 1e-08

def sequence_layout(lengths):
    pack_rows = jnp.arange(PACK, dtype=jnp.int32)

    def one_pack(row_lengths):
        offsets = (jnp.cumsum(row_lengths) - row_lengths).astype(jnp.int32)
        covered = pack_rows[:, None] >= offsets[None, :]
        seq_ids = lax.optimization_barrier(jnp.sum(covered.astype(jnp.int32), axis=1)).astype(jnp.int32) - 1
        starts = lax.optimization_barrier(jnp.max(jnp.where(covered, offsets[None, :], 0), axis=1)).astype(jnp.int32)
        return (seq_ids, pack_rows - starts)
    seq_ids, positions = jax.vmap(one_pack)(lengths)
    return (seq_ids.reshape(-1), positions.reshape(-1))

def rope_tables(positions):
    half_width = ROT // 2
    inverse = jnp.power(ROPE_BASE, -jnp.arange(half_width, dtype=jnp.float32) * (2.0 / ROT))
    angles = positions.astype(jnp.float32)[:, None] * inverse[None, :]
    return (jnp.cos(angles), jnp.sin(angles))

def rotate(vectors, cosine, sine):
    half_width = ROT // 2
    leading = vectors[..., :half_width]
    trailing = vectors[..., half_width:ROT]
    cosine_rows = cosine[:, None, :]
    sine_rows = sine[:, None, :]
    return jnp.concatenate([leading * cosine_rows - trailing * sine_rows, trailing * cosine_rows + leading * sine_rows, vectors[..., ROT:]], axis=-1)

def attention(queries, keys_all, values_all, seq_ids):
    block_rows = min(512, PACK)
    block_count = PACK // block_rows
    window_rows = LONGEST + block_rows
    pack_shape = (N_REP, PACK, HEADS, HEAD_DIM)
    padding = ((0, 0), (LONGEST, 0), (0, 0), (0, 0))
    query_pack = queries.reshape(pack_shape)
    key_pack = jnp.pad(keys_all.reshape(pack_shape), padding)
    value_pack = jnp.pad(values_all.reshape(pack_shape), padding)
    seq_pack = jnp.pad(seq_ids.reshape(N_REP, PACK), ((0, 0), (LONGEST, 0)), constant_values=-1)

    def one_block(block_id):
        pack_at = block_id // block_count
        row_first = block_id % block_count * block_rows
        anchor = jnp.zeros((), jnp.int32)
        query_block = lax.dynamic_slice(query_pack, (pack_at, row_first, anchor, anchor), (1, block_rows, HEADS, HEAD_DIM))[0]
        key_block = lax.dynamic_slice(key_pack, (pack_at, row_first, anchor, anchor), (1, window_rows, HEADS, HEAD_DIM))[0]
        value_block = lax.dynamic_slice(value_pack, (pack_at, row_first, anchor, anchor), (1, window_rows, HEADS, HEAD_DIM))[0]
        query_seq = lax.dynamic_slice(seq_pack, (pack_at, row_first + LONGEST), (1, block_rows))[0]
        key_seq = lax.dynamic_slice(seq_pack, (pack_at, row_first), (1, window_rows))[0]
        query_row = row_first + jnp.arange(block_rows, dtype=jnp.int32)
        key_row = row_first - LONGEST + jnp.arange(window_rows, dtype=jnp.int32)
        allowed = (key_seq[None, :] == query_seq[:, None]) & (key_row[None, :] <= query_row[:, None])
        scores = low_back(jnp.einsum('qhe,khe->hqk', query_block, key_block, precision=PRECISE) * HEAD_DIM ** (-0.5))
        scores = jnp.where(allowed[None], scores, NEG_LARGE)
        probs = low(jax.nn.softmax(scores, axis=-1))
        return jnp.einsum('hqk,khe->qhe', probs, value_block, precision=PRECISE).reshape(block_rows, HEADS * HEAD_DIM)
    blocks_out = lax.map(jax.checkpoint(one_block), jnp.arange(N_REP * block_count, dtype=jnp.int32))
    return blocks_out.reshape(N_REP * PACK, HEADS * HEAD_DIM)

def forward(params, given, placement, seq_ids, positions):
    norm_gain, norm_bias, project_weight, project_bias, output_weight, output_bias, expand_weight, expand_bias, reduce_weight, reduce_bias = params
    row_total = given.shape[0]
    inverse = jnp.zeros((row_total,), jnp.int32).at[placement].set(jnp.arange(row_total, dtype=jnp.int32))
    packed = given[inverse]
    row_mean = lax.optimization_barrier(jnp.mean(packed, axis=1, keepdims=True))
    centred = packed - row_mean
    row_var = lax.optimization_barrier(jnp.mean(centred * centred, axis=1, keepdims=True))
    normed = low(centred * lax.rsqrt(row_var + NORM_EPSILON) * norm_gain + norm_bias)
    joined = jnp.dot(normed, low(project_weight), precision=PRECISE) + project_bias
    joined = low_back(joined).reshape(row_total, HEADS, 3, HEAD_DIM)
    cosine, sine = rope_tables(positions)
    queries = low(rotate(joined[:, :, 0], cosine, sine))
    keys_all = low(rotate(joined[:, :, 1], cosine, sine))
    values_all = low(joined[:, :, 2])
    attended = low(low_back(attention(queries, keys_all, values_all, seq_ids)))
    hidden = low_back(jnp.dot(normed, low(expand_weight), precision=PRECISE) + expand_bias)
    activated = low(jax.nn.gelu(hidden, approximate=True))
    attn_branch = jnp.dot(attended, low(output_weight), precision=PRECISE) + output_bias
    feed_branch = jnp.dot(activated, low(reduce_weight), precision=PRECISE) + reduce_bias
    packed_out = packed + attn_branch + feed_branch
    return packed_out[placement]

def newton_schulz(blocks):
    gram = jnp.einsum('bik,bjk->bij', blocks, blocks, precision=PRECISE)
    factor = lax.rsqrt(jnp.trace(gram, axis1=1, axis2=2) + SCHULZ_EPSILON)
    current = blocks * factor[:, None, None]
    gram = gram * (factor * factor)[:, None, None]
    for turn_id in range(SCHULZ_STEPS):
        if turn_id > 0:
            gram = jnp.einsum('bik,bjk->bij', current, current, precision=PRECISE)
        mixing = SCHULZ_SECOND * gram + SCHULZ_THIRD * jnp.einsum('bij,bjk->bik', gram, gram, precision=PRECISE)
        current = SCHULZ_FIRST * current + jnp.einsum('bij,bjk->bik', mixing, current, precision=PRECISE)
    return current

def row_blocks(matrix):
    return matrix.reshape(N_FSDP, matrix.shape[0] // N_FSDP, matrix.shape[1])

def from_row_blocks(blocks):
    return blocks.reshape(-1, blocks.shape[2])

def column_blocks(matrix):
    return matrix.reshape(matrix.shape[0], N_FSDP, matrix.shape[1] // N_FSDP).transpose(1, 2, 0)

def from_column_blocks(blocks):
    return blocks.transpose(2, 0, 1).reshape(blocks.shape[2], -1)

def muon_update(weight, momentum, gradient, to_blocks, from_blocks, long_side):
    momentum_new = MUON_DECAY * momentum + gradient
    ortho = from_blocks(newton_schulz(to_blocks(momentum_new)))
    weight_new = weight - MUON_RATE * (RMS_MATCH * math.sqrt(long_side) * ortho + WEIGHT_DECAY * weight)
    return (weight_new, weight_new.astype(jnp.bfloat16), momentum_new)

def adam_update(param, first_moment, second_moment, gradient, step_count):
    moment_one = ADAM_FIRST * first_moment + (1.0 - ADAM_FIRST) * gradient
    moment_two = ADAM_SECOND * second_moment + (1.0 - ADAM_SECOND) * gradient * gradient
    step_value = step_count[0].astype(jnp.float32)
    one_fixed = moment_one / (1.0 - ADAM_FIRST ** step_value)
    two_fixed = moment_two / (1.0 - ADAM_SECOND ** step_value)
    param_new = param - ADAM_RATE * one_fixed / (jnp.sqrt(two_fixed) + ADAM_EPSILON)
    return (param_new, moment_one, moment_two)

def reference(tokens, cotangent, placement, lengths, step_count, norm_gain, norm_bias, project_weight, project_bias, output_weight, output_bias, expand_weight, expand_bias, reduce_weight, reduce_bias, project_momentum, output_momentum, expand_momentum, reduce_momentum, norm_gain_first, norm_gain_second, norm_bias_first, norm_bias_second, project_bias_first, project_bias_second, output_bias_first, output_bias_second, expand_bias_first, expand_bias_second, reduce_bias_first, reduce_bias_second):
    seq_ids, positions = sequence_layout(lengths)
    params = (norm_gain, norm_bias, project_weight, project_bias, output_weight, output_bias, expand_weight, expand_bias, reduce_weight, reduce_bias)

    def wrapped(weights_all, given):
        return forward(weights_all, given, placement, seq_ids, positions)
    result, pullback = jax.vjp(wrapped, params, tokens.astype(jnp.float32))
    param_grads, input_grad = pullback(cotangent.astype(jnp.float32))
    norm_gain_grad, norm_bias_grad, project_weight_grad, project_bias_grad, output_weight_grad, output_bias_grad, expand_weight_grad, expand_bias_grad, reduce_weight_grad, reduce_bias_grad = param_grads
    project_new, project_copy, project_mom = muon_update(project_weight, project_momentum, project_weight_grad, row_blocks, from_row_blocks, 3 * D)
    output_new, output_copy, output_mom = muon_update(output_weight, output_momentum, output_weight_grad, column_blocks, from_column_blocks, D)
    expand_new, expand_copy, expand_mom = muon_update(expand_weight, expand_momentum, expand_weight_grad, row_blocks, from_row_blocks, FF)
    reduce_new, reduce_copy, reduce_mom = muon_update(reduce_weight, reduce_momentum, reduce_weight_grad, column_blocks, from_column_blocks, FF)
    gain_new, gain_one, gain_two = adam_update(norm_gain, norm_gain_first, norm_gain_second, norm_gain_grad, step_count)
    shift_new, shift_one, shift_two = adam_update(norm_bias, norm_bias_first, norm_bias_second, norm_bias_grad, step_count)
    pbias_new, pbias_one, pbias_two = adam_update(project_bias, project_bias_first, project_bias_second, project_bias_grad, step_count)
    obias_new, obias_one, obias_two = adam_update(output_bias, output_bias_first, output_bias_second, output_bias_grad, step_count)
    ebias_new, ebias_one, ebias_two = adam_update(expand_bias, expand_bias_first, expand_bias_second, expand_bias_grad, step_count)
    rbias_new, rbias_one, rbias_two = adam_update(reduce_bias, reduce_bias_first, reduce_bias_second, reduce_bias_grad, step_count)
    return (result.astype(jnp.bfloat16), input_grad.astype(jnp.bfloat16), norm_gain_grad, norm_bias_grad, project_weight_grad, project_bias_grad, output_weight_grad, output_bias_grad, expand_weight_grad, expand_bias_grad, reduce_weight_grad, reduce_bias_grad, gain_new, shift_new, project_new, pbias_new, output_new, obias_new, expand_new, ebias_new, reduce_new, rbias_new, project_copy, output_copy, expand_copy, reduce_copy, project_mom, output_mom, expand_mom, reduce_mom, gain_one, gain_two, shift_one, shift_two, pbias_one, pbias_two, obias_one, obias_two, ebias_one, ebias_two, rbias_one, rbias_two)
```

```python
import functools
import math

import jax
import jax.numpy as jnp
from jax import lax
from jax.experimental import pallas as pl
from jax.experimental.pallas import tpu as pltpu
from jax.sharding import PartitionSpec as P

D = 2048
HEAD_DIM = 64
ROT = 32
FF = 8192
SCHULZ_STEPS = 5


NORM_EPSILON = 1e-05
ROPE_BASE = 10000.0
NEG_LARGE = -1e30
SCHULZ_FIRST = 3.4445
SCHULZ_SECOND = -4.775
SCHULZ_THIRD = 2.0315
SCHULZ_EPSILON = 1e-06
MUON_RATE = 0.2
MUON_DECAY = 0.5
RMS_MATCH = 0.2
WEIGHT_DECAY = 0.1
ADAM_RATE = 0.2
ADAM_FIRST = 0.9
ADAM_SECOND = 0.95
ADAM_EPSILON = 1e-08


def sequence_layout(row_lengths, row_ids):
    offsets = jnp.cumsum(row_lengths) - row_lengths
    covered = row_ids[:, None] >= offsets[None, :]
    seq_ids = jnp.sum(covered.astype(jnp.int32), axis=1) - 1
    starts = jnp.max(jnp.where(covered, offsets[None, :], 0), axis=1)
    return (seq_ids, starts)


def rope_tables(positions):
    half_width = ROT // 2
    inverse = jnp.power(ROPE_BASE, -jnp.arange(half_width, dtype=jnp.float32) * (2.0 / ROT))
    angles = positions.astype(jnp.float32)[:, None] * inverse[None, :]
    return (jnp.cos(angles), jnp.sin(angles))


def rotate(vectors, cosine, sine):
    half_width = ROT // 2
    leading = vectors[..., :half_width]
    trailing = vectors[..., half_width:ROT]
    cosine_rows = cosine[:, None, :]
    sine_rows = sine[:, None, :]
    return jnp.concatenate(
        [
            leading * cosine_rows - trailing * sine_rows,
            trailing * cosine_rows + leading * sine_rows,
            vectors[..., ROT:],
        ],
        axis=-1,
    )


def layer_norm(rows_in, gain_vector, shift_vector):
    row_mean = jnp.mean(rows_in, axis=1, keepdims=True)
    centred = rows_in - row_mean
    row_var = jnp.mean(centred * centred, axis=1, keepdims=True)
    return centred * lax.rsqrt(row_var + NORM_EPSILON) * gain_vector + shift_vector


def gelu_tanh(values_in):
    return jax.nn.gelu(values_in, approximate=True)


def local_gram(block_part):
    return jnp.einsum("ik,jk->ij", block_part, block_part, precision=lax.Precision.HIGHEST)


def schulz_turn(block_part, gram_sum):
    mixing = SCHULZ_SECOND * gram_sum + SCHULZ_THIRD * jnp.dot(
        gram_sum, gram_sum, precision=lax.Precision.HIGHEST
    )
    return SCHULZ_FIRST * block_part + jnp.dot(mixing, block_part, precision=lax.Precision.HIGHEST)


def muon_weight(weight, ortho, long_side):
    return weight - MUON_RATE * (RMS_MATCH * math.sqrt(long_side) * ortho + WEIGHT_DECAY * weight)


def adam_update(param, first_moment, second_moment, gradient, step_count):
    moment_one = ADAM_FIRST * first_moment + (1.0 - ADAM_FIRST) * gradient
    moment_two = ADAM_SECOND * second_moment + (1.0 - ADAM_SECOND) * gradient * gradient
    step_value = step_count[0].astype(jnp.float32)
    one_fixed = moment_one / (1.0 - ADAM_FIRST**step_value)
    two_fixed = moment_two / (1.0 - ADAM_SECOND**step_value)
    param_new = param - ADAM_RATE * one_fixed / (jnp.sqrt(two_fixed) + ADAM_EPSILON)
    return (param_new, moment_one, moment_two)


BLOCK = 256
LANES = 128


def dot_nt(left, right):
    return lax.dot_general(
        left, right, (((1,), (1,)), ((), ())), preferred_element_type=jnp.float32
    )


def dot_nn(left, right):
    return lax.dot_general(
        left, right, (((1,), (0,)), ((), ())), preferred_element_type=jnp.float32
    )


def turn_pairs(values, cosine, sine):
    lane = lax.broadcasted_iota(jnp.int32, values.shape, 1) % HEAD_DIM
    width = values.shape[1]
    ahead = pltpu.roll(values, width - ROT // 2, 1)
    behind = pltpu.roll(values, ROT // 2, 1)
    return values * cosine + jnp.where(lane < ROT // 2, ahead, behind) * sine


def rope_body(joined_ref, cosine_ref, sine_ref, q_ref, k_ref, v_ref, kt_ref, vt_ref):
    rows = joined_ref[...].reshape(BLOCK, 3 * LANES)
    cosine, sine = cosine_ref[...], sine_ref[...]
    queries = turn_pairs(rows[:, :LANES], cosine, sine).astype(jnp.bfloat16)
    q_ref[...] = queries * jnp.bfloat16(HEAD_DIM**-0.5)
    keys = turn_pairs(rows[:, LANES : 2 * LANES], cosine, sine)
    k_ref[...] = keys.astype(jnp.bfloat16)
    kt_ref[...] = keys.T.astype(jnp.bfloat16)
    values = rows[:, 2 * LANES :]
    v_ref[...] = values.astype(jnp.bfloat16)
    vt_ref[...] = values.T.astype(jnp.bfloat16)


def unrope_body(dq_ref, dk_ref, dv_ref, cosine_ref, sine_ref, out_ref, sum_ref):
    cosine, sine = cosine_ref[...], -sine_ref[...]
    parts = (
        turn_pairs(dq_ref[...], cosine, sine),
        turn_pairs(dk_ref[...], cosine, sine),
        dv_ref[...],
    )

    @pl.when((pl.program_id(0) == 0) & (pl.program_id(1) == 0))
    def _():
        sum_ref[...] = jnp.zeros_like(sum_ref)

    for part_at, part in enumerate(parts):
        low = part.astype(jnp.bfloat16)
        cols = slice(part_at * LANES, (part_at + 1) * LANES)
        out_ref[..., cols] = low.reshape(out_ref.shape[:-1] + (LANES,))
        wide = low.astype(jnp.float32).reshape(BLOCK // 8, 8, LANES)
        sum_ref[:, cols] += jnp.sum(wide, axis=0)


def sequence_starts(lengths_ref, row_ids):
    offset = jnp.int32(0)
    starts = jnp.zeros_like(row_ids)
    for seq_at in range(lengths_ref.shape[0] - 1):
        offset = offset + lengths_ref[seq_at]
        starts = jnp.where(row_ids >= offset, offset, starts)
    return starts


def first_block(lengths_ref, block_at):
    row = block_at * BLOCK
    offset = jnp.int32(0)
    start = jnp.int32(0)
    for seq_at in range(lengths_ref.shape[0] - 1):
        offset = offset + lengths_ref[seq_at]
        start = jnp.where(row >= offset, offset, start)
    return start // BLOCK


def head_lanes(values, head):
    lane = lax.broadcasted_iota(jnp.int32, values.shape, 1)
    return jnp.where(lane // HEAD_DIM == head, values, jnp.zeros_like(values))


def masked_scores(key_ref, queries, key_block, query_ids, starts):
    first = pl.multiple_of(key_block * BLOCK, BLOCK)
    scores = dot_nt(key_ref[pl.ds(first, BLOCK), :], queries)
    key_ids = first + lax.broadcasted_iota(jnp.int32, (BLOCK, BLOCK), 0)
    allowed = (key_ids >= starts) & (key_ids <= query_ids)
    return jnp.where(allowed, scores, NEG_LARGE)


def attend_body(lengths_ref, q_ref, k_ref, vt_ref, out_ref, stat_ref, held):
    block_at = pl.program_id(0) * pl.num_programs(1) + pl.program_id(1)
    begin = first_block(lengths_ref, block_at)
    query_ids = block_at * BLOCK + lax.broadcasted_iota(jnp.int32, (1, BLOCK), 1)
    starts = sequence_starts(lengths_ref, query_ids)
    queries = q_ref[...]
    outs = []
    for head in range(LANES // HEAD_DIM):
        one = head_lanes(queries, head)

        def score_step(key_block, top):
            scores = masked_scores(k_ref, one, key_block, query_ids, starts)
            held[key_block] = scores
            return jnp.maximum(top, jnp.max(scores, axis=0, keepdims=True))

        top = lax.fori_loop(
            begin, block_at + 1, score_step, jnp.full((1, BLOCK), NEG_LARGE, jnp.float32)
        )

        def total_step(key_block, total):
            raised = jnp.exp(held[key_block] - top)
            held[key_block] = raised
            return total + jnp.sum(raised, axis=0, keepdims=True)

        total = lax.fori_loop(
            begin, block_at + 1, total_step, jnp.zeros((1, BLOCK), jnp.float32)
        )
        inverse = 1.0 / total

        def value_step(key_block, accum):
            first = pl.multiple_of(key_block * BLOCK, BLOCK)
            probs_low = (held[key_block] * inverse).astype(jnp.bfloat16)
            return accum + dot_nn(vt_ref[:, pl.ds(first, BLOCK)], probs_low)

        accum = lax.fori_loop(
            begin, block_at + 1, value_step, jnp.zeros((LANES, BLOCK), jnp.float32)
        )
        outs.append(accum)
        stat_ref[pl.ds(head, 1), :] = top + jnp.log(total)
    row = lax.broadcasted_iota(jnp.int32, (LANES, BLOCK), 0)
    merged = jnp.where(row < HEAD_DIM, outs[0], outs[1])
    out_ref[...] = merged.T.astype(jnp.bfloat16).reshape(out_ref.shape)


def attend_back_body(
    lengths_ref,
    q_ref,
    grad_ref,
    stat_ref,
    k_ref,
    v_ref,
    kt_ref,
    dq_ref,
    dk_ref,
    dv_ref,
    held_probs,
    held_grads,
):
    block_at = pl.program_id(0) * pl.num_programs(1) + pl.program_id(1)

    @pl.when(block_at == 0)
    def _():
        dk_ref[...] = jnp.zeros_like(dk_ref)
        dv_ref[...] = jnp.zeros_like(dv_ref)

    begin = first_block(lengths_ref, block_at)
    query_ids = block_at * BLOCK + lax.broadcasted_iota(jnp.int32, (1, BLOCK), 1)
    starts = sequence_starts(lengths_ref, query_ids)
    queries = q_ref[...]
    grads = grad_ref[...].reshape(BLOCK, LANES)
    outs = []
    for head in range(LANES // HEAD_DIM):
        one = head_lanes(queries, head)
        one_grad = head_lanes(grads, head)
        log_total = stat_ref[pl.ds(head, 1), :]

        def probs_step(key_block, delta):
            first = pl.multiple_of(key_block * BLOCK, BLOCK)
            scores = masked_scores(k_ref, one, key_block, query_ids, starts)
            probs = jnp.exp(scores - log_total)
            d_probs = dot_nt(v_ref[pl.ds(first, BLOCK), :], one_grad)
            held_probs[key_block] = probs
            held_grads[key_block] = d_probs
            return delta + jnp.sum(probs * d_probs, axis=0, keepdims=True)

        delta = lax.fori_loop(
            begin, block_at + 1, probs_step, jnp.zeros((1, BLOCK), jnp.float32)
        )

        def grads_step(key_block, accum):
            first = pl.multiple_of(key_block * BLOCK, BLOCK)
            rows = pl.ds(first, BLOCK)
            probs = held_probs[key_block]
            d_scores = (probs * (held_grads[key_block] - delta)).astype(jnp.bfloat16)
            dk_ref[rows, :] += dot_nn(d_scores, one)
            dv_ref[rows, :] += dot_nn(probs.astype(jnp.bfloat16), one_grad)
            return accum + dot_nn(kt_ref[:, rows], d_scores)

        outs.append(
            lax.fori_loop(
                begin, block_at + 1, grads_step, jnp.zeros((LANES, BLOCK), jnp.float32)
            )
        )
    row = lax.broadcasted_iota(jnp.int32, (LANES, BLOCK), 0)
    merged = jnp.where(row < HEAD_DIM, outs[0], outs[1])
    dq_ref[...] = merged.T * HEAD_DIM**-0.5


def given_block(dealt, groups, slot, width):
    return pl.BlockSpec((dealt, 1, 1, slot, width), lambda d, n, *_: (0, n, d, 0, 0))


def rope(joined, cosine, sine, dealt, groups):
    rows = joined.shape[0]
    slot = rows // (dealt * groups * dealt)
    view = joined.reshape(dealt, groups, dealt, slot, 3 * LANES)
    flat = pl.BlockSpec((BLOCK, LANES), lambda d, n: (d * groups + n, 0))
    turned = pl.BlockSpec((LANES, BLOCK), lambda d, n: (0, d * groups + n))
    straight = jax.ShapeDtypeStruct((rows, LANES), jnp.bfloat16)
    across = jax.ShapeDtypeStruct((LANES, rows), jnp.bfloat16)
    return pl.pallas_call(
        rope_body,
        grid=(dealt, groups),
        in_specs=[given_block(dealt, groups, slot, 3 * LANES), flat, flat],
        out_specs=[flat, flat, flat, turned, turned],
        out_shape=[straight, straight, straight, across, across],
        cost_estimate=pl.CostEstimate(
            flops=rows * LANES * 12, bytes_accessed=rows * LANES * 30, transcendentals=0
        ),
        name="rope",
    )(view, cosine, sine)


def unrope(d_queries, d_keys, d_values, cosine, sine, dealt, groups):
    rows = d_queries.shape[0]
    slot = rows // (dealt * groups * dealt)
    flat = pl.BlockSpec((BLOCK, LANES), lambda d, n: (d * groups + n, 0))
    out, sums = pl.pallas_call(
        unrope_body,
        grid=(dealt, groups),
        in_specs=[flat] * 5,
        out_specs=[
            given_block(dealt, groups, slot, 3 * LANES),
            pl.BlockSpec((8, 3 * LANES), lambda d, n: (0, 0)),
        ],
        out_shape=[
            jax.ShapeDtypeStruct((dealt, groups, dealt, slot, 3 * LANES), jnp.bfloat16),
            jax.ShapeDtypeStruct((8, 3 * LANES), jnp.float32),
        ],
        cost_estimate=pl.CostEstimate(
            flops=rows * LANES * 12, bytes_accessed=rows * LANES * 26, transcendentals=0
        ),
        name="unrope",
    )(d_queries, d_keys, d_values, cosine, sine)
    return out.reshape(rows, 3 * LANES), jnp.sum(sums, axis=0)


def attend(row_lengths, queries, keys, values_turned, dealt, groups):
    rows = queries.shape[0]
    slot = rows // (dealt * groups * dealt)
    flat = pl.BlockSpec((BLOCK, LANES), lambda d, n, _: (d * groups + n, 0))
    attended, stats = pl.pallas_call(
        attend_body,
        grid_spec=pltpu.PrefetchScalarGridSpec(
            num_scalar_prefetch=1,
            grid=(dealt, groups),
            in_specs=[
                flat,
                pl.BlockSpec((rows, LANES), lambda d, n, _: (0, 0)),
                pl.BlockSpec((LANES, rows), lambda d, n, _: (0, 0)),
            ],
            out_specs=[
                given_block(dealt, groups, slot, LANES),
                pl.BlockSpec((8, BLOCK), lambda d, n, _: (0, d * groups + n)),
            ],
            scratch_shapes=[pltpu.VMEM((rows // BLOCK, BLOCK, BLOCK), jnp.float32)],
        ),
        out_shape=[
            jax.ShapeDtypeStruct((dealt, groups, dealt, slot, LANES), jnp.bfloat16),
            jax.ShapeDtypeStruct((8, rows), jnp.float32),
        ],
        cost_estimate=pl.CostEstimate(
            flops=rows * rows * LANES * 2,
            bytes_accessed=rows * LANES * 10,
            transcendentals=rows * rows // 2,
        ),
        name="attend",
    )(row_lengths, queries, keys, values_turned)
    return attended.reshape(rows, LANES), stats


def attend_back(row_lengths, queries, grads, stats, keys, values, keys_turned, dealt, groups):
    rows = queries.shape[0]
    slot = rows // (dealt * groups * dealt)
    flat = pl.BlockSpec((BLOCK, LANES), lambda d, n, _: (d * groups + n, 0))
    whole = pl.BlockSpec((rows, LANES), lambda d, n, _: (0, 0))
    wide = jax.ShapeDtypeStruct((rows, LANES), jnp.float32)
    return pl.pallas_call(
        attend_back_body,
        grid_spec=pltpu.PrefetchScalarGridSpec(
            num_scalar_prefetch=1,
            grid=(dealt, groups),
            in_specs=[
                flat,
                given_block(dealt, groups, slot, LANES),
                pl.BlockSpec((8, BLOCK), lambda d, n, _: (0, d * groups + n)),
                whole,
                whole,
                pl.BlockSpec((LANES, rows), lambda d, n, _: (0, 0)),
            ],
            out_specs=[flat, whole, whole],
            scratch_shapes=[pltpu.VMEM((rows // BLOCK, BLOCK, BLOCK), jnp.float32)] * 2,
        ),
        out_shape=[wide, wide, wide],
        cost_estimate=pl.CostEstimate(
            flops=rows * rows * LANES * 4,
            bytes_accessed=rows * LANES * 24,
            transcendentals=rows * rows // 2,
        ),
        name="attend_back",
    )(
        row_lengths,
        queries,
        grads.reshape(dealt, groups, dealt, slot, LANES),
        stats,
        keys,
        values,
        keys_turned,
    )


def gelu_slope(values_in):
    scale = math.sqrt(2.0 / math.pi)
    bent = jnp.tanh(scale * (values_in + 0.044715 * values_in * values_in * values_in))
    return 0.5 * (1.0 + bent) + 0.5 * values_in * (1.0 - bent * bent) * scale * (
        1.0 + 3.0 * 0.044715 * values_in * values_in
    )


def schulz_chain(gram):
    precise = functools.partial(jnp.dot, precision=lax.Precision.HIGHEST)
    eye = jnp.eye(gram.shape[0], dtype=jnp.float32)
    chain = None
    for turn_id in range(SCHULZ_STEPS):
        turn = (
            SCHULZ_FIRST * eye + SCHULZ_SECOND * gram + SCHULZ_THIRD * precise(gram, gram)
        )
        chain = turn if chain is None else precise(turn, chain)
        if turn_id < SCHULZ_STEPS - 1:
            gram = precise(precise(turn, gram), turn)
    return chain


def gathered_weights(
    tokens,
    cotangent,
    placement,
    lengths,
    step_count,
    norm_gain,
    norm_bias,
    project_weight,
    project_bias,
    output_weight,
    output_bias,
    expand_weight,
    expand_bias,
    reduce_weight,
    reduce_bias,
    project_momentum,
    output_momentum,
    expand_momentum,
    reduce_momentum,
    norm_gain_first,
    norm_gain_second,
    norm_bias_first,
    norm_bias_second,
    project_bias_first,
    project_bias_second,
    output_bias_first,
    output_bias_second,
    expand_bias_first,
    expand_bias_second,
    reduce_bias_first,
    reduce_bias_second,
):
    fsdp_count = lax.axis_size("fsdp")
    ns_count = lax.axis_size("ns")
    shard_rows = tokens.shape[0]
    slot_rows = shard_rows // fsdp_count
    group_rows = shard_rows * ns_count
    pack_rows = group_rows * fsdp_count
    fsdp_at = lax.axis_index("fsdp")
    ns_at = lax.axis_index("ns")
    row_lengths = lengths[0]
    heads_here = project_bias.shape[0] // (3 * HEAD_DIM)
    head_cols = heads_here * HEAD_DIM
    scale_factor = HEAD_DIM ** (-0.5)
    within = placement % shard_rows
    dest_fsdp = placement // shard_rows // ns_count % fsdp_count
    slot_index = dest_fsdp * slot_rows + within - fsdp_at * slot_rows
    source_row = (
        jnp.zeros((shard_rows,), jnp.int32)
        .at[slot_index]
        .set(jnp.arange(shard_rows, dtype=jnp.int32))
    )
    dealt_tokens, dealt_cotangent = (
        lax.all_to_all(tokens[source_row], "fsdp", split_axis=0, concat_axis=0, tiled=True),
        lax.all_to_all(cotangent[source_row], "fsdp", split_axis=0, concat_axis=0, tiled=True),
    )
    token_rows = dealt_tokens.astype(jnp.float32)
    normed, norm_back = jax.vjp(layer_norm, token_rows, norm_gain, norm_bias)
    normed_low = normed.astype(jnp.bfloat16)
    normed_all, cotangent_all = (
        lax.all_gather(normed_low, "ns", axis=0, tiled=True),
        lax.all_gather(dealt_cotangent, "ns", axis=0, tiled=True),
    )
    project_low = project_weight.astype(jnp.bfloat16)
    output_low = output_weight.astype(jnp.bfloat16)
    expand_low = expand_weight.astype(jnp.bfloat16)
    reduce_low = reduce_weight.astype(jnp.bfloat16)
    project_full, output_full, expand_full, reduce_full = (
        lax.all_gather(project_low, "fsdp", axis=0, tiled=True),
        lax.all_gather(output_low, "fsdp", axis=1, tiled=True),
        lax.all_gather(expand_low, "fsdp", axis=0, tiled=True),
        lax.all_gather(reduce_low, "fsdp", axis=1, tiled=True),
    )
    group_first = fsdp_at * group_rows
    query_rows = group_first + jnp.arange(group_rows, dtype=jnp.int32)
    query_seq, query_starts = sequence_layout(row_lengths, query_rows)
    positions = query_rows - query_starts
    reach_first = query_starts[0]
    query_last = group_first + group_rows - 1
    cosine, sine = rope_tables(positions)
    joined = jnp.dot(normed_all, project_full, preferred_element_type=jnp.float32) + project_bias
    joined = joined.reshape(group_rows, heads_here, 3, HEAD_DIM)
    query_view = rotate(joined[:, :, 0], cosine, sine).astype(jnp.bfloat16)
    keys_here = (
        rotate(joined[:, :, 1], cosine, sine).astype(jnp.bfloat16).reshape(group_rows, head_cols)
    )
    values_here = joined[:, :, 2].astype(jnp.bfloat16).reshape(group_rows, head_cols)
    paired_here = jnp.stack([keys_here, values_here], axis=1)

    def wanted(key_first, key_count):
        return (key_first <= query_last) & (key_first + key_count - 1 >= reach_first)

    def piece_scores(key_piece, key_first):
        key_count = key_piece.shape[0]
        key_rows = key_first + jnp.arange(key_count, dtype=jnp.int32)
        key_seq = sequence_layout(row_lengths, key_rows)[0]
        scores = (
            jnp.einsum(
                "qhe,khe->hqk",
                query_view,
                key_piece.reshape(key_count, heads_here, HEAD_DIM),
                preferred_element_type=jnp.float32,
            )
            * scale_factor
        )
        allowed = (key_seq[None, :] == query_seq[:, None]) & (
            key_rows[None, :] <= query_rows[:, None]
        )
        return jnp.where(allowed[None], scores, NEG_LARGE)

    paired_group = lax.all_gather(paired_here, "fsdp", axis=0, tiled=True)
    paired_stack = paired_group.reshape(fsdp_count, group_rows, 2, head_cols)
    first_rows = jnp.arange(fsdp_count, dtype=jnp.int32) * group_rows

    def sweep(step_fn, initial):

        def scan_body(running, scan_item):
            return step_fn(running, scan_item[0][:, 0], scan_item[0][:, 1], scan_item[1])

        return lax.scan(scan_body, initial, (paired_stack, first_rows))

    def stats_step(running, key_piece, value_piece, key_first):

        def stats_compute(held_stats):
            row_top, row_sum = held_stats
            scores = piece_scores(key_piece, key_first)
            top_new = jnp.maximum(row_top, jnp.max(scores, axis=2))
            sum_new = row_sum * jnp.exp(row_top - top_new) + jnp.sum(
                jnp.exp(scores - top_new[:, :, None]), axis=2
            )
            return (top_new, sum_new)

        return (
            lax.cond(
                wanted(key_first, key_piece.shape[0]),
                stats_compute,
                lambda held_stats: held_stats,
                running,
            ),
            None,
        )

    initial_stats = (
        jnp.full((heads_here, group_rows), NEG_LARGE, jnp.float32),
        jnp.zeros((heads_here, group_rows), jnp.float32),
    )
    final_stats = sweep(stats_step, initial_stats)[0]
    log_total = final_stats[0] + jnp.log(final_stats[1])

    def output_step(running, key_piece, value_piece, key_first):
        key_count = key_piece.shape[0]

        def output_compute(accum):
            scores = piece_scores(key_piece, key_first)
            probs_low = jnp.exp(scores - log_total[:, :, None]).astype(jnp.bfloat16)
            return accum + jnp.einsum(
                "hqk,khe->qhe",
                probs_low,
                value_piece.reshape(key_count, heads_here, HEAD_DIM),
                preferred_element_type=jnp.float32,
            )

        return (
            lax.cond(wanted(key_first, key_count), output_compute, lambda accum: accum, running),
            None,
        )

    attended = sweep(output_step, jnp.zeros((group_rows, heads_here, HEAD_DIM), jnp.float32))[0]
    attended_low = attended.reshape(group_rows, head_cols).astype(jnp.bfloat16)
    hidden = jnp.dot(normed_all, expand_full, preferred_element_type=jnp.float32) + expand_bias
    activated, gelu_back = jax.vjp(gelu_tanh, hidden)
    activated_low = activated.astype(jnp.bfloat16)
    branch_sum = lax.psum_scatter(
        jnp.dot(attended_low, output_full, preferred_element_type=jnp.float32)
        + jnp.dot(activated_low, reduce_full, preferred_element_type=jnp.float32),
        "ns",
        scatter_dimension=0,
        tiled=True,
    )
    layer_rows = (token_rows + branch_sum + output_bias + reduce_bias).astype(jnp.bfloat16)
    back_project, back_output, back_expand, back_reduce = (
        lax.all_gather(project_low, "fsdp", axis=0, tiled=True),
        lax.all_gather(output_low, "fsdp", axis=1, tiled=True),
        lax.all_gather(expand_low, "fsdp", axis=0, tiled=True),
        lax.all_gather(reduce_low, "fsdp", axis=1, tiled=True),
    )
    d_attended = jnp.einsum(
        "td,hd->th", cotangent_all, back_output, preferred_element_type=jnp.float32
    ).astype(jnp.bfloat16)
    d_attended_view = d_attended.reshape(group_rows, heads_here, HEAD_DIM)
    d_activated = jnp.einsum(
        "td,fd->tf", cotangent_all, back_reduce, preferred_element_type=jnp.float32
    )
    d_hidden = gelu_back(d_activated)[0].astype(jnp.bfloat16)

    def delta_step(running, key_piece, value_piece, key_first):
        key_count = key_piece.shape[0]

        def delta_compute(accum):
            scores = piece_scores(key_piece, key_first)
            probs = jnp.exp(scores - log_total[:, :, None])
            d_probs = jnp.einsum(
                "qhe,khe->hqk",
                d_attended_view,
                value_piece.reshape(key_count, heads_here, HEAD_DIM),
                preferred_element_type=jnp.float32,
            )
            return accum + jnp.sum(probs * d_probs, axis=2)

        return (
            lax.cond(wanted(key_first, key_count), delta_compute, lambda accum: accum, running),
            None,
        )

    delta = sweep(delta_step, jnp.zeros((heads_here, group_rows), jnp.float32))[0]

    def grads_step(running, key_piece, value_piece, key_first):
        key_count = key_piece.shape[0]

        def grads_compute(d_queries):
            keys_view = key_piece.reshape(key_count, heads_here, HEAD_DIM)
            values_view = value_piece.reshape(key_count, heads_here, HEAD_DIM)
            scores = piece_scores(key_piece, key_first)
            probs = jnp.exp(scores - log_total[:, :, None])
            d_probs = jnp.einsum(
                "qhe,khe->hqk", d_attended_view, values_view, preferred_element_type=jnp.float32
            )
            d_scores = (probs * (d_probs - delta[:, :, None])).astype(jnp.bfloat16)
            d_queries = (
                d_queries
                + jnp.einsum(
                    "hqk,khe->qhe", d_scores, keys_view, preferred_element_type=jnp.float32
                )
                * scale_factor
            )
            d_keys = (
                jnp.einsum("hqk,qhe->khe", d_scores, query_view, preferred_element_type=jnp.float32)
                * scale_factor
            )
            d_values = jnp.einsum(
                "hqk,qhe->khe",
                probs.astype(jnp.bfloat16),
                d_attended_view,
                preferred_element_type=jnp.float32,
            )
            return (
                d_queries,
                jnp.stack(
                    [d_keys.reshape(key_count, head_cols), d_values.reshape(key_count, head_cols)],
                    axis=1,
                ),
            )

        def skipped(d_queries):
            return (d_queries, jnp.zeros((key_count, 2, head_cols), jnp.float32))

        return lax.cond(wanted(key_first, key_count), grads_compute, skipped, running)

    d_queries, key_extras = sweep(
        grads_step, jnp.zeros((group_rows, heads_here, HEAD_DIM), jnp.float32)
    )
    key_sums = lax.psum_scatter(
        key_extras.reshape(pack_rows, 2, head_cols), "fsdp", scatter_dimension=0, tiled=True
    )
    d_keys_own = key_sums[:, 0].reshape(group_rows, heads_here, HEAD_DIM)
    d_values_own = key_sums[:, 1].reshape(group_rows, heads_here, HEAD_DIM)
    d_joined = jnp.stack(
        [rotate(d_queries, cosine, -sine), rotate(d_keys_own, cosine, -sine), d_values_own], axis=2
    )
    d_joined = d_joined.reshape(group_rows, 3 * head_cols).astype(jnp.bfloat16)
    d_normed = lax.psum_scatter(
        jnp.einsum("tc,dc->td", d_joined, back_project, preferred_element_type=jnp.float32)
        + jnp.einsum("tf,df->td", d_hidden, back_expand, preferred_element_type=jnp.float32),
        "ns",
        scatter_dimension=0,
        tiled=True,
    )
    d_tokens_norm, gain_term, shift_term = norm_back(d_normed)
    input_rows = (dealt_cotangent.astype(jnp.float32) + d_tokens_norm).astype(jnp.bfloat16)
    back_layer, back_input = (
        lax.all_to_all(layer_rows, "fsdp", split_axis=0, concat_axis=0, tiled=True),
        lax.all_to_all(input_rows, "fsdp", split_axis=0, concat_axis=0, tiled=True),
    )
    layer_output = back_layer[slot_index]
    input_grad = back_input[slot_index]
    project_term = jnp.einsum("td,tc->dc", normed_all, d_joined, preferred_element_type=jnp.float32)
    output_term = jnp.einsum(
        "th,td->hd", attended_low, cotangent_all, preferred_element_type=jnp.float32
    )
    expand_term = jnp.einsum("td,tf->df", normed_all, d_hidden, preferred_element_type=jnp.float32)
    reduce_term = jnp.einsum(
        "tf,td->fd", activated_low, cotangent_all, preferred_element_type=jnp.float32
    )
    shards = (
        lax.psum_scatter(project_term, "fsdp", scatter_dimension=0, tiled=True),
        lax.psum_scatter(output_term, "fsdp", scatter_dimension=1, tiled=True),
        lax.psum_scatter(expand_term, "fsdp", scatter_dimension=0, tiled=True),
        lax.psum_scatter(reduce_term, "fsdp", scatter_dimension=1, tiled=True),
    )
    project_grad, output_grad, expand_grad, reduce_grad = lax.psum(
        (shards[0], shards[1], shards[2], shards[3]), "rep"
    )
    project_bias_width = project_bias.shape[0]
    expand_bias_width = expand_bias.shape[0]
    project_bias_part = lax.dynamic_update_slice(
        jnp.zeros((project_bias_width * ns_count,), jnp.float32),
        jnp.sum(d_joined, axis=0, dtype=jnp.float32),
        (ns_at * project_bias_width,),
    )
    expand_bias_part = lax.dynamic_update_slice(
        jnp.zeros((expand_bias_width * ns_count,), jnp.float32),
        jnp.sum(d_hidden, axis=0, dtype=jnp.float32),
        (ns_at * expand_bias_width,),
    )
    cotangent_sum = jnp.sum(dealt_cotangent, axis=0, dtype=jnp.float32)
    gain_grad, shift_grad, cotangent_total, project_bias_all, expand_bias_all = lax.psum(
        (gain_term, shift_term, cotangent_sum, project_bias_part, expand_bias_part),
        ("rep", "fsdp", "ns"),
    )
    project_bias_grad = lax.dynamic_slice_in_dim(
        project_bias_all, ns_at * project_bias_width, project_bias_width
    )
    expand_bias_grad = lax.dynamic_slice_in_dim(
        expand_bias_all, ns_at * expand_bias_width, expand_bias_width
    )
    project_mom = MUON_DECAY * project_momentum + project_grad
    output_mom = MUON_DECAY * output_momentum + output_grad
    expand_mom = MUON_DECAY * expand_momentum + expand_grad
    reduce_mom = MUON_DECAY * reduce_momentum + reduce_grad
    current = (project_mom, output_mom.T, expand_mom, reduce_mom.T)
    for turn_id in range(SCHULZ_STEPS):
        grams = lax.psum(
            (
                local_gram(current[0]),
                local_gram(current[1]),
                local_gram(current[2]),
                local_gram(current[3]),
            ),
            "ns",
        )
        if turn_id == 0:
            factors = [lax.rsqrt(jnp.trace(gram_sum) + SCHULZ_EPSILON) for gram_sum in grams]
            current = tuple(
                (block_part * factor_now for block_part, factor_now in zip(current, factors))
            )
            grams = tuple(
                (
                    gram_sum * (factor_now * factor_now)
                    for gram_sum, factor_now in zip(grams, factors)
                )
            )
        current = tuple(
            (schulz_turn(block_part, gram_sum) for block_part, gram_sum in zip(current, grams))
        )
    project_new = muon_weight(project_weight, current[0], 3 * D)
    output_new = muon_weight(output_weight, current[1].T, D)
    expand_new = muon_weight(expand_weight, current[2], FF)
    reduce_new = muon_weight(reduce_weight, current[3].T, FF)
    gain_new, gain_one, gain_two = adam_update(
        norm_gain, norm_gain_first, norm_gain_second, gain_grad, step_count
    )
    shift_new, shift_one, shift_two = adam_update(
        norm_bias, norm_bias_first, norm_bias_second, shift_grad, step_count
    )
    pbias_new, pbias_one, pbias_two = adam_update(
        project_bias, project_bias_first, project_bias_second, project_bias_grad, step_count
    )
    obias_new, obias_one, obias_two = adam_update(
        output_bias, output_bias_first, output_bias_second, cotangent_total, step_count
    )
    ebias_new, ebias_one, ebias_two = adam_update(
        expand_bias, expand_bias_first, expand_bias_second, expand_bias_grad, step_count
    )
    rbias_new, rbias_one, rbias_two = adam_update(
        reduce_bias, reduce_bias_first, reduce_bias_second, cotangent_total, step_count
    )
    return (
        layer_output,
        input_grad,
        gain_grad,
        shift_grad,
        project_grad,
        project_bias_grad,
        output_grad,
        cotangent_total,
        expand_grad,
        expand_bias_grad,
        reduce_grad,
        cotangent_total,
        gain_new,
        shift_new,
        project_new,
        pbias_new,
        output_new,
        obias_new,
        expand_new,
        ebias_new,
        reduce_new,
        rbias_new,
        project_new.astype(jnp.bfloat16),
        output_new.astype(jnp.bfloat16),
        expand_new.astype(jnp.bfloat16),
        reduce_new.astype(jnp.bfloat16),
        project_mom,
        output_mom,
        expand_mom,
        reduce_mom,
        gain_one,
        gain_two,
        shift_one,
        shift_two,
        pbias_one,
        pbias_two,
        obias_one,
        obias_two,
        ebias_one,
        ebias_two,
        rbias_one,
        rbias_two,
    )


def per_device(axis_sizes, *arguments):
    heads = arguments[8].shape[0] // (3 * HEAD_DIM)
    shard_rows = arguments[0].shape[0]
    dealt = axis_sizes["fsdp"]
    fits = heads * HEAD_DIM == dealt * LANES and shard_rows == BLOCK and BLOCK % (8 * dealt) == 0
    return (split_heads if fits else gathered_weights)(*arguments)


def split_heads(
    tokens,
    cotangent,
    placement,
    lengths,
    step_count,
    norm_gain,
    norm_bias,
    project_weight,
    project_bias,
    output_weight,
    output_bias,
    expand_weight,
    expand_bias,
    reduce_weight,
    reduce_bias,
    project_momentum,
    output_momentum,
    expand_momentum,
    reduce_momentum,
    norm_gain_first,
    norm_gain_second,
    norm_bias_first,
    norm_bias_second,
    project_bias_first,
    project_bias_second,
    output_bias_first,
    output_bias_second,
    expand_bias_first,
    expand_bias_second,
    reduce_bias_first,
    reduce_bias_second,
):
    dealt = lax.axis_size("fsdp")
    groups = lax.axis_size("ns")
    shard_rows = tokens.shape[0]
    slot = shard_rows // dealt
    pack_rows = shard_rows * dealt * groups
    fsdp_at = lax.axis_index("fsdp")
    ns_at = lax.axis_index("ns")
    row_lengths = lengths[0]
    low = jnp.bfloat16

    within = placement % shard_rows
    dest = placement // shard_rows // groups % dealt
    slot_index = dest * slot + within - fsdp_at * slot
    slots = jnp.arange(shard_rows, dtype=jnp.int32)
    deal = (slot_index[None, :] == slots[:, None]).astype(low)
    sorted_tokens = jnp.dot(deal, tokens, preferred_element_type=jnp.float32)
    sorted_cotangent = jnp.dot(deal, cotangent, preferred_element_type=jnp.float32).astype(low)
    normed, norm_back = jax.vjp(layer_norm, sorted_tokens, norm_gain, norm_bias)
    normed_all = lax.all_gather(normed.astype(low), ("fsdp", "ns"), axis=0, tiled=True)
    cotangent_all = lax.all_gather(sorted_cotangent, ("fsdp", "ns"), axis=0, tiled=True)

    def exchange(pieces):
        return lax.all_to_all(pieces, "fsdp", split_axis=0, concat_axis=0, tiled=True)

    col = jnp.arange(3 * LANES, dtype=jnp.int32)
    dest_col = (
        col % (3 * HEAD_DIM) // HEAD_DIM * LANES
        + col // (3 * HEAD_DIM) * HEAD_DIM
        + col % HEAD_DIM
    )
    shuffle = (dest_col[:, None] == col[None, :]).astype(low)
    width = project_weight.shape[0]
    ff_here = expand_bias.shape[0] // dealt
    project_pieces = jnp.einsum(
        "rfc,cd->frd",
        project_weight.astype(low).reshape(width, dealt, 3 * LANES),
        shuffle,
        preferred_element_type=low,
    )
    project_full = exchange(project_pieces).reshape(dealt * width, 3 * LANES)
    expand_pieces = expand_weight.astype(low).reshape(width, dealt, ff_here).transpose(1, 0, 2)
    expand_full = exchange(expand_pieces).reshape(dealt * width, ff_here)
    output_pieces = output_weight.astype(low).reshape(dealt, LANES, width)
    output_full = exchange(output_pieces).transpose(1, 0, 2).reshape(LANES, dealt * width)
    reduce_pieces = reduce_weight.astype(low).reshape(dealt, ff_here, width)
    reduce_full = exchange(reduce_pieces).transpose(1, 0, 2).reshape(ff_here, dealt * width)

    pack_ids = jnp.arange(pack_rows, dtype=jnp.int32)
    positions = pack_ids - sequence_layout(row_lengths, pack_ids)[1]
    cosine_half, sine_half = rope_tables(positions)
    still = jnp.zeros((pack_rows, HEAD_DIM - ROT), jnp.float32)
    head_cosine = jnp.concatenate([cosine_half, cosine_half, still + 1.0], axis=1)
    head_sine = jnp.concatenate([-sine_half, sine_half, still], axis=1)
    cosine = jnp.concatenate([head_cosine, head_cosine], axis=1)
    sine = jnp.concatenate([head_sine, head_sine], axis=1)

    project_bias_here = lax.dynamic_slice_in_dim(project_bias, fsdp_at * 3 * LANES, 3 * LANES)
    project_bias_here = (
        project_bias_here.reshape(-1, 3, HEAD_DIM).transpose(1, 0, 2).reshape(3 * LANES)
    )
    expand_bias_here = lax.dynamic_slice_in_dim(expand_bias, fsdp_at * ff_here, ff_here)
    joined = (
        jnp.dot(normed_all, project_full, preferred_element_type=jnp.float32) + project_bias_here
    )
    queries, keys, values, keys_turned, values_turned = rope(joined, cosine, sine, dealt, groups)
    attended_low, stats = attend(row_lengths, queries, keys, values_turned, dealt, groups)
    hidden = jnp.dot(normed_all, expand_full, preferred_element_type=jnp.float32) + expand_bias_here
    activated_low = gelu_tanh(hidden).astype(low)
    branch = jnp.dot(attended_low, output_full, preferred_element_type=jnp.float32) + jnp.dot(
        activated_low, reduce_full, preferred_element_type=jnp.float32
    )
    branch_sum = lax.psum_scatter(
        branch.astype(low), ("fsdp", "ns"), scatter_dimension=0, tiled=True
    ).astype(jnp.float32)
    layer_rows = (sorted_tokens + branch_sum + output_bias + reduce_bias).astype(low)

    d_attended = dot_nt(cotangent_all, output_full).astype(low)
    d_hidden = (gelu_slope(hidden) * dot_nt(cotangent_all, reduce_full)).astype(low)
    d_queries, d_keys, d_values = attend_back(
        row_lengths, queries, d_attended, stats, keys, values, keys_turned, dealt, groups
    )
    d_joined, d_joined_sum = unrope(d_queries, d_keys, d_values, cosine, sine, dealt, groups)
    d_normed_part = dot_nt(d_joined, project_full) + dot_nt(d_hidden, expand_full)
    d_normed = lax.psum_scatter(
        d_normed_part.astype(low), ("fsdp", "ns"), scatter_dimension=0, tiled=True
    ).astype(jnp.float32)
    d_tokens_norm, gain_term, shift_term = norm_back(d_normed)
    input_rows = (sorted_cotangent.astype(jnp.float32) + d_tokens_norm).astype(low)

    def undeal(rows):
        return lax.dot_general(
            deal, rows, (((0,), (0,)), ((), ())), preferred_element_type=jnp.float32
        ).astype(low)

    layer_output = undeal(layer_rows)
    input_grad = undeal(input_rows)

    def outer(left, right):
        return lax.dot_general(
            left, right, (((0,), (0,)), ((), ())), preferred_element_type=jnp.float32
        ).astype(low)

    def both_packs(shard):
        twin = lax.ppermute(shard, "rep", [(0, 1), (1, 0)]) if lax.axis_size("rep") == 2 else None
        if twin is None:
            return lax.psum(shard.astype(jnp.float32), "rep")
        return shard.astype(jnp.float32) + twin.astype(jnp.float32)

    reduce_term = outer(activated_low, cotangent_all).reshape(ff_here, dealt, width)
    reduce_grad = both_packs(
        exchange(reduce_term.transpose(1, 0, 2)).reshape(dealt * ff_here, width)
    )
    output_term = outer(attended_low, cotangent_all).reshape(LANES, dealt, width)
    output_grad = both_packs(
        exchange(output_term.transpose(1, 0, 2)).reshape(dealt * LANES, width)
    )
    expand_term = outer(normed_all, d_hidden).reshape(dealt, width, ff_here)
    expand_grad = both_packs(
        exchange(expand_term).transpose(1, 0, 2).reshape(width, dealt * ff_here)
    )
    project_term = jnp.einsum(
        "frd,cd->frc",
        outer(normed_all, d_joined).reshape(dealt, width, 3 * LANES),
        shuffle,
        preferred_element_type=low,
    )
    project_grad = both_packs(
        exchange(project_term).transpose(1, 0, 2).reshape(width, dealt * 3 * LANES)
    )

    part_at = ns_at * dealt + fsdp_at
    project_bias_width = project_bias.shape[0]
    expand_bias_width = expand_bias.shape[0]
    project_bias_part = lax.dynamic_update_slice(
        jnp.zeros((project_bias_width * groups,), jnp.float32),
        d_joined_sum.reshape(3, -1, HEAD_DIM).transpose(1, 0, 2).reshape(3 * LANES),
        (part_at * 3 * LANES,),
    )
    expand_bias_part = lax.dynamic_update_slice(
        jnp.zeros((expand_bias_width * groups,), jnp.float32),
        jnp.sum(d_hidden, axis=0, dtype=jnp.float32),
        (part_at * ff_here,),
    )
    cotangent_sum = jnp.sum(sorted_cotangent, axis=0, dtype=jnp.float32)
    gain_grad, shift_grad, cotangent_total, project_bias_all, expand_bias_all = lax.psum(
        (gain_term, shift_term, cotangent_sum, project_bias_part, expand_bias_part),
        ("rep", "fsdp", "ns"),
    )
    project_bias_grad = lax.dynamic_slice_in_dim(
        project_bias_all, ns_at * project_bias_width, project_bias_width
    )
    expand_bias_grad = lax.dynamic_slice_in_dim(
        expand_bias_all, ns_at * expand_bias_width, expand_bias_width
    )

    project_mom = MUON_DECAY * project_momentum + project_grad
    output_mom = MUON_DECAY * output_momentum + output_grad
    expand_mom = MUON_DECAY * expand_momentum + expand_grad
    reduce_mom = MUON_DECAY * reduce_momentum + reduce_grad
    precise = functools.partial(lax.dot_general, precision=lax.Precision.HIGHEST)
    by_row = (((1,), (1,)), ((), ()))
    by_col = (((0,), (0,)), ((), ()))
    grams = jnp.stack(
        [
            precise(project_mom, project_mom, by_row),
            precise(output_mom, output_mom, by_col),
            precise(expand_mom, expand_mom, by_row),
            precise(reduce_mom, reduce_mom, by_col),
        ]
    )
    gram = lax.psum_scatter(grams, "ns", scatter_dimension=0, tiled=True)[0]
    factor = lax.rsqrt(jnp.trace(gram) + SCHULZ_EPSILON)
    chain = schulz_chain(gram * (factor * factor)) * factor
    chains = lax.all_gather(chain, "ns", axis=0)
    left = (((1,), (0,)), ((), ()))
    right = (((1,), (1,)), ((), ()))
    project_new = muon_weight(project_weight, precise(chains[0], project_mom, left), 3 * D)
    output_new = muon_weight(output_weight, precise(output_mom, chains[1], right), D)
    expand_new = muon_weight(expand_weight, precise(chains[2], expand_mom, left), FF)
    reduce_new = muon_weight(reduce_weight, precise(reduce_mom, chains[3], right), FF)

    gain_new, gain_one, gain_two = adam_update(
        norm_gain, norm_gain_first, norm_gain_second, gain_grad, step_count
    )
    shift_new, shift_one, shift_two = adam_update(
        norm_bias, norm_bias_first, norm_bias_second, shift_grad, step_count
    )
    pbias_new, pbias_one, pbias_two = adam_update(
        project_bias, project_bias_first, project_bias_second, project_bias_grad, step_count
    )
    obias_new, obias_one, obias_two = adam_update(
        output_bias, output_bias_first, output_bias_second, cotangent_total, step_count
    )
    ebias_new, ebias_one, ebias_two = adam_update(
        expand_bias, expand_bias_first, expand_bias_second, expand_bias_grad, step_count
    )
    rbias_new, rbias_one, rbias_two = adam_update(
        reduce_bias, reduce_bias_first, reduce_bias_second, cotangent_total, step_count
    )
    return (
        layer_output,
        input_grad,
        gain_grad,
        shift_grad,
        project_grad,
        project_bias_grad,
        output_grad,
        cotangent_total,
        expand_grad,
        expand_bias_grad,
        reduce_grad,
        cotangent_total,
        gain_new,
        shift_new,
        project_new,
        pbias_new,
        output_new,
        obias_new,
        expand_new,
        ebias_new,
        reduce_new,
        rbias_new,
        project_new.astype(jnp.bfloat16),
        output_new.astype(jnp.bfloat16),
        expand_new.astype(jnp.bfloat16),
        reduce_new.astype(jnp.bfloat16),
        project_mom,
        output_mom,
        expand_mom,
        reduce_mom,
        gain_one,
        gain_two,
        shift_one,
        shift_two,
        pbias_one,
        pbias_two,
        obias_one,
        obias_two,
        ebias_one,
        ebias_two,
        rbias_one,
        rbias_two,
    )


def solution(mesh):
    return jax.shard_map(
        functools.partial(per_device, dict(mesh.shape)),
        mesh=mesh,
        in_specs=(
            P(("rep", "fsdp", "ns"), None),
            P(("rep", "fsdp", "ns"), None),
            P(("rep", "fsdp", "ns")),
            P("rep", None),
            P(),
            P(),
            P(),
            P("fsdp", "ns"),
            P("ns"),
            P("ns", "fsdp"),
            P(),
            P("fsdp", "ns"),
            P("ns"),
            P("ns", "fsdp"),
            P(),
            P("fsdp", "ns"),
            P("ns", "fsdp"),
            P("fsdp", "ns"),
            P("ns", "fsdp"),
            P(),
            P(),
            P(),
            P(),
            P("ns"),
            P("ns"),
            P(),
            P(),
            P("ns"),
            P("ns"),
            P(),
            P(),
        ),
        out_specs=(
            P(("rep", "fsdp", "ns"), None),
            P(("rep", "fsdp", "ns"), None),
            P(),
            P(),
            P("fsdp", "ns"),
            P("ns"),
            P("ns", "fsdp"),
            P(),
            P("fsdp", "ns"),
            P("ns"),
            P("ns", "fsdp"),
            P(),
            P(),
            P(),
            P("fsdp", "ns"),
            P("ns"),
            P("ns", "fsdp"),
            P(),
            P("fsdp", "ns"),
            P("ns"),
            P("ns", "fsdp"),
            P(),
            P("fsdp", "ns"),
            P("ns", "fsdp"),
            P("fsdp", "ns"),
            P("ns", "fsdp"),
            P("fsdp", "ns"),
            P("ns", "fsdp"),
            P("fsdp", "ns"),
            P("ns", "fsdp"),
            P(),
            P(),
            P(),
            P(),
            P("ns"),
            P("ns"),
            P(),
            P(),
            P("ns"),
            P("ns"),
            P(),
            P(),
        ),
        check_vma=False,
    )
```

```python
import functools
import math

import jax
import jax.numpy as jnp
from jax import lax
from jax.experimental import pallas as pl
from jax.experimental.pallas import tpu as pltpu
from jax.sharding import PartitionSpec as P

D = 2048
HEAD_DIM = 64
ROT = 32
FF = 8192
SCHULZ_STEPS = 5


NORM_EPSILON = 1e-05
ROPE_BASE = 10000.0
NEG_LARGE = -1e30
SCHULZ_FIRST = 3.4445
SCHULZ_SECOND = -4.775
SCHULZ_THIRD = 2.0315
SCHULZ_EPSILON = 1e-06
MUON_RATE = 0.2
MUON_DECAY = 0.5
RMS_MATCH = 0.2
WEIGHT_DECAY = 0.1
ADAM_RATE = 0.2
ADAM_FIRST = 0.9
ADAM_SECOND = 0.95
ADAM_EPSILON = 1e-08


def sequence_layout(row_lengths, row_ids):
    offsets = jnp.cumsum(row_lengths) - row_lengths
    covered = row_ids[:, None] >= offsets[None, :]
    seq_ids = jnp.sum(covered.astype(jnp.int32), axis=1) - 1
    starts = jnp.max(jnp.where(covered, offsets[None, :], 0), axis=1)
    return (seq_ids, starts)


def rope_tables(positions):
    half_width = ROT // 2
    inverse = jnp.power(ROPE_BASE, -jnp.arange(half_width, dtype=jnp.float32) * (2.0 / ROT))
    angles = positions.astype(jnp.float32)[:, None] * inverse[None, :]
    return (jnp.cos(angles), jnp.sin(angles))


def rotate(vectors, cosine, sine):
    half_width = ROT // 2
    leading = vectors[..., :half_width]
    trailing = vectors[..., half_width:ROT]
    cosine_rows = cosine[:, None, :]
    sine_rows = sine[:, None, :]
    return jnp.concatenate(
        [
            leading * cosine_rows - trailing * sine_rows,
            trailing * cosine_rows + leading * sine_rows,
            vectors[..., ROT:],
        ],
        axis=-1,
    )


def layer_norm(rows_in, gain_vector, shift_vector):
    row_mean = jnp.mean(rows_in, axis=1, keepdims=True)
    centred = rows_in - row_mean
    row_var = jnp.mean(centred * centred, axis=1, keepdims=True)
    return centred * lax.rsqrt(row_var + NORM_EPSILON) * gain_vector + shift_vector


def gelu_tanh(values_in):
    return jax.nn.gelu(values_in, approximate=True)


def local_gram(block_part):
    return jnp.einsum("ik,jk->ij", block_part, block_part, precision=lax.Precision.HIGHEST)


def schulz_turn(block_part, gram_sum):
    mixing = SCHULZ_SECOND * gram_sum + SCHULZ_THIRD * jnp.dot(
        gram_sum, gram_sum, precision=lax.Precision.HIGHEST
    )
    return SCHULZ_FIRST * block_part + jnp.dot(mixing, block_part, precision=lax.Precision.HIGHEST)


def muon_weight(weight, ortho, long_side):
    return weight - MUON_RATE * (RMS_MATCH * math.sqrt(long_side) * ortho + WEIGHT_DECAY * weight)


def adam_update(param, first_moment, second_moment, gradient, step_count):
    moment_one = ADAM_FIRST * first_moment + (1.0 - ADAM_FIRST) * gradient
    moment_two = ADAM_SECOND * second_moment + (1.0 - ADAM_SECOND) * gradient * gradient
    step_value = step_count[0].astype(jnp.float32)
    one_fixed = moment_one / (1.0 - ADAM_FIRST**step_value)
    two_fixed = moment_two / (1.0 - ADAM_SECOND**step_value)
    param_new = param - ADAM_RATE * one_fixed / (jnp.sqrt(two_fixed) + ADAM_EPSILON)
    return (param_new, moment_one, moment_two)


BLOCK = 256
LANES = 128


def dot_nt(left, right):
    return lax.dot_general(
        left, right, (((1,), (1,)), ((), ())), preferred_element_type=jnp.float32
    )


def dot_nn(left, right):
    return lax.dot_general(
        left, right, (((1,), (0,)), ((), ())), preferred_element_type=jnp.float32
    )


def turn_pairs(values, cosine, sine):
    lane = lax.broadcasted_iota(jnp.int32, values.shape, 1) % HEAD_DIM
    width = values.shape[1]
    ahead = pltpu.roll(values, width - ROT // 2, 1)
    behind = pltpu.roll(values, ROT // 2, 1)
    return values * cosine + jnp.where(lane < ROT // 2, ahead, behind) * sine


def rope_body(joined_ref, cosine_ref, sine_ref, q_ref, k_ref, v_ref, kt_ref, vt_ref):
    rows = joined_ref[...].reshape(BLOCK, 3 * LANES)
    cosine, sine = cosine_ref[...], sine_ref[...]
    queries = turn_pairs(rows[:, :LANES], cosine, sine).astype(jnp.bfloat16)
    q_ref[...] = queries * jnp.bfloat16(HEAD_DIM**-0.5)
    keys = turn_pairs(rows[:, LANES : 2 * LANES], cosine, sine)
    k_ref[...] = keys.astype(jnp.bfloat16)
    kt_ref[...] = keys.T.astype(jnp.bfloat16)
    values = rows[:, 2 * LANES :]
    v_ref[...] = values.astype(jnp.bfloat16)
    vt_ref[...] = values.T.astype(jnp.bfloat16)


def unrope_body(dq_ref, dk_ref, dv_ref, cosine_ref, sine_ref, out_ref, sum_ref):
    cosine, sine = cosine_ref[...], -sine_ref[...]
    parts = (
        turn_pairs(dq_ref[...], cosine, sine),
        turn_pairs(dk_ref[...], cosine, sine),
        dv_ref[...],
    )

    @pl.when((pl.program_id(0) == 0) & (pl.program_id(1) == 0))
    def _():
        sum_ref[...] = jnp.zeros_like(sum_ref)

    for part_at, part in enumerate(parts):
        low = part.astype(jnp.bfloat16)
        cols = slice(part_at * LANES, (part_at + 1) * LANES)
        out_ref[..., cols] = low.reshape(out_ref.shape[:-1] + (LANES,))
        wide = low.astype(jnp.float32).reshape(BLOCK // 8, 8, LANES)
        sum_ref[:, cols] += jnp.sum(wide, axis=0)


def sequence_starts(lengths_ref, row_ids):
    offset = jnp.int32(0)
    starts = jnp.zeros_like(row_ids)
    for seq_at in range(lengths_ref.shape[0] - 1):
        offset = offset + lengths_ref[seq_at]
        starts = jnp.where(row_ids >= offset, offset, starts)
    return starts


def first_block(lengths_ref, block_at):
    row = block_at * BLOCK
    offset = jnp.int32(0)
    start = jnp.int32(0)
    for seq_at in range(lengths_ref.shape[0] - 1):
        offset = offset + lengths_ref[seq_at]
        start = jnp.where(row >= offset, offset, start)
    return start // BLOCK


def head_lanes(values, head):
    lane = lax.broadcasted_iota(jnp.int32, values.shape, 1)
    return jnp.where(lane // HEAD_DIM == head, values, jnp.zeros_like(values))


def masked_scores(key_ref, queries, key_block, query_ids, starts):
    first = pl.multiple_of(key_block * BLOCK, BLOCK)
    scores = dot_nt(key_ref[pl.ds(first, BLOCK), :], queries)
    key_ids = first + lax.broadcasted_iota(jnp.int32, (BLOCK, BLOCK), 0)
    allowed = (key_ids >= starts) & (key_ids <= query_ids)
    return jnp.where(allowed, scores, NEG_LARGE)


def attend_body(lengths_ref, q_ref, k_ref, vt_ref, out_ref, stat_ref, held):
    block_at = pl.program_id(0) * pl.num_programs(1) + pl.program_id(1)
    begin = first_block(lengths_ref, block_at)
    query_ids = block_at * BLOCK + lax.broadcasted_iota(jnp.int32, (1, BLOCK), 1)
    starts = sequence_starts(lengths_ref, query_ids)
    queries = q_ref[...]
    outs = []
    for head in range(LANES // HEAD_DIM):
        one = head_lanes(queries, head)

        def score_step(key_block, top):
            scores = masked_scores(k_ref, one, key_block, query_ids, starts)
            held[key_block] = scores
            return jnp.maximum(top, jnp.max(scores, axis=0, keepdims=True))

        top = lax.fori_loop(
            begin, block_at + 1, score_step, jnp.full((1, BLOCK), NEG_LARGE, jnp.float32)
        )

        def total_step(key_block, total):
            raised = jnp.exp(held[key_block] - top)
            held[key_block] = raised
            return total + jnp.sum(raised, axis=0, keepdims=True)

        total = lax.fori_loop(
            begin, block_at + 1, total_step, jnp.zeros((1, BLOCK), jnp.float32)
        )
        inverse = 1.0 / total

        def value_step(key_block, accum):
            first = pl.multiple_of(key_block * BLOCK, BLOCK)
            probs_low = (held[key_block] * inverse).astype(jnp.bfloat16)
            return accum + dot_nn(vt_ref[:, pl.ds(first, BLOCK)], probs_low)

        accum = lax.fori_loop(
            begin, block_at + 1, value_step, jnp.zeros((LANES, BLOCK), jnp.float32)
        )
        outs.append(accum)
        stat_ref[pl.ds(head, 1), :] = top + jnp.log(total)
    row = lax.broadcasted_iota(jnp.int32, (LANES, BLOCK), 0)
    merged = jnp.where(row < HEAD_DIM, outs[0], outs[1])
    out_ref[...] = merged.T.astype(jnp.bfloat16).reshape(out_ref.shape)


def attend_back_body(
    lengths_ref,
    q_ref,
    grad_ref,
    stat_ref,
    k_ref,
    v_ref,
    kt_ref,
    dq_ref,
    dk_ref,
    dv_ref,
    held_probs,
    held_grads,
):
    block_at = pl.program_id(0) * pl.num_programs(1) + pl.program_id(1)

    @pl.when(block_at == 0)
    def _():
        dk_ref[...] = jnp.zeros_like(dk_ref)
        dv_ref[...] = jnp.zeros_like(dv_ref)

    begin = first_block(lengths_ref, block_at)
    query_ids = block_at * BLOCK + lax.broadcasted_iota(jnp.int32, (1, BLOCK), 1)
    starts = sequence_starts(lengths_ref, query_ids)
    queries = q_ref[...]
    grads = grad_ref[...].reshape(BLOCK, LANES)
    outs = []
    for head in range(LANES // HEAD_DIM):
        one = head_lanes(queries, head)
        one_grad = head_lanes(grads, head)
        log_total = stat_ref[pl.ds(head, 1), :]

        def probs_step(key_block, delta):
            first = pl.multiple_of(key_block * BLOCK, BLOCK)
            scores = masked_scores(k_ref, one, key_block, query_ids, starts)
            probs = jnp.exp(scores - log_total)
            d_probs = dot_nt(v_ref[pl.ds(first, BLOCK), :], one_grad)
            held_probs[key_block] = probs
            held_grads[key_block] = d_probs
            return delta + jnp.sum(probs * d_probs, axis=0, keepdims=True)

        delta = lax.fori_loop(
            begin, block_at + 1, probs_step, jnp.zeros((1, BLOCK), jnp.float32)
        )

        def grads_step(key_block, accum):
            first = pl.multiple_of(key_block * BLOCK, BLOCK)
            rows = pl.ds(first, BLOCK)
            probs = held_probs[key_block]
            d_scores = (probs * (held_grads[key_block] - delta)).astype(jnp.bfloat16)
            dk_ref[rows, :] += dot_nn(d_scores, one)
            dv_ref[rows, :] += dot_nn(probs.astype(jnp.bfloat16), one_grad)
            return accum + dot_nn(kt_ref[:, rows], d_scores)

        outs.append(
            lax.fori_loop(
                begin, block_at + 1, grads_step, jnp.zeros((LANES, BLOCK), jnp.float32)
            )
        )
    row = lax.broadcasted_iota(jnp.int32, (LANES, BLOCK), 0)
    merged = jnp.where(row < HEAD_DIM, outs[0], outs[1])
    dq_ref[...] = merged.T * HEAD_DIM**-0.5


def given_block(dealt, groups, slot, width):
    return pl.BlockSpec((dealt, 1, 1, slot, width), lambda d, n, *_: (0, n, d, 0, 0))


def rope(joined, cosine, sine, dealt, groups):
    rows = joined.shape[0]
    slot = rows // (dealt * groups * dealt)
    view = joined.reshape(dealt, groups, dealt, slot, 3 * LANES)
    flat = pl.BlockSpec((BLOCK, LANES), lambda d, n: (d * groups + n, 0))
    turned = pl.BlockSpec((LANES, BLOCK), lambda d, n: (0, d * groups + n))
    straight = jax.ShapeDtypeStruct((rows, LANES), jnp.bfloat16)
    across = jax.ShapeDtypeStruct((LANES, rows), jnp.bfloat16)
    return pl.pallas_call(
        rope_body,
        grid=(dealt, groups),
        in_specs=[given_block(dealt, groups, slot, 3 * LANES), flat, flat],
        out_specs=[flat, flat, flat, turned, turned],
        out_shape=[straight, straight, straight, across, across],
        cost_estimate=pl.CostEstimate(
            flops=rows * LANES * 12, bytes_accessed=rows * LANES * 30, transcendentals=0
        ),
        name="rope",
    )(view, cosine, sine)


def unrope(d_queries, d_keys, d_values, cosine, sine, dealt, groups):
    rows = d_queries.shape[0]
    slot = rows // (dealt * groups * dealt)
    flat = pl.BlockSpec((BLOCK, LANES), lambda d, n: (d * groups + n, 0))
    out, sums = pl.pallas_call(
        unrope_body,
        grid=(dealt, groups),
        in_specs=[flat] * 5,
        out_specs=[
            given_block(dealt, groups, slot, 3 * LANES),
            pl.BlockSpec((8, 3 * LANES), lambda d, n: (0, 0)),
        ],
        out_shape=[
            jax.ShapeDtypeStruct((dealt, groups, dealt, slot, 3 * LANES), jnp.bfloat16),
            jax.ShapeDtypeStruct((8, 3 * LANES), jnp.float32),
        ],
        cost_estimate=pl.CostEstimate(
            flops=rows * LANES * 12, bytes_accessed=rows * LANES * 26, transcendentals=0
        ),
        name="unrope",
    )(d_queries, d_keys, d_values, cosine, sine)
    return out.reshape(rows, 3 * LANES), jnp.sum(sums, axis=0)


def attend(row_lengths, queries, keys, values_turned, dealt, groups):
    rows = queries.shape[0]
    slot = rows // (dealt * groups * dealt)
    flat = pl.BlockSpec((BLOCK, LANES), lambda d, n, _: (d * groups + n, 0))
    attended, stats = pl.pallas_call(
        attend_body,
        grid_spec=pltpu.PrefetchScalarGridSpec(
            num_scalar_prefetch=1,
            grid=(dealt, groups),
            in_specs=[
                flat,
                pl.BlockSpec((rows, LANES), lambda d, n, _: (0, 0)),
                pl.BlockSpec((LANES, rows), lambda d, n, _: (0, 0)),
            ],
            out_specs=[
                given_block(dealt, groups, slot, LANES),
                pl.BlockSpec((8, BLOCK), lambda d, n, _: (0, d * groups + n)),
            ],
            scratch_shapes=[pltpu.VMEM((rows // BLOCK, BLOCK, BLOCK), jnp.float32)],
        ),
        out_shape=[
            jax.ShapeDtypeStruct((dealt, groups, dealt, slot, LANES), jnp.bfloat16),
            jax.ShapeDtypeStruct((8, rows), jnp.float32),
        ],
        cost_estimate=pl.CostEstimate(
            flops=rows * rows * LANES * 2,
            bytes_accessed=rows * LANES * 10,
            transcendentals=rows * rows // 2,
        ),
        name="attend",
    )(row_lengths, queries, keys, values_turned)
    return attended.reshape(rows, LANES), stats


def attend_back(row_lengths, queries, grads, stats, keys, values, keys_turned, dealt, groups):
    rows = queries.shape[0]
    slot = rows // (dealt * groups * dealt)
    flat = pl.BlockSpec((BLOCK, LANES), lambda d, n, _: (d * groups + n, 0))
    whole = pl.BlockSpec((rows, LANES), lambda d, n, _: (0, 0))
    wide = jax.ShapeDtypeStruct((rows, LANES), jnp.float32)
    return pl.pallas_call(
        attend_back_body,
        grid_spec=pltpu.PrefetchScalarGridSpec(
            num_scalar_prefetch=1,
            grid=(dealt, groups),
            in_specs=[
                flat,
                given_block(dealt, groups, slot, LANES),
                pl.BlockSpec((8, BLOCK), lambda d, n, _: (0, d * groups + n)),
                whole,
                whole,
                pl.BlockSpec((LANES, rows), lambda d, n, _: (0, 0)),
            ],
            out_specs=[flat, whole, whole],
            scratch_shapes=[pltpu.VMEM((rows // BLOCK, BLOCK, BLOCK), jnp.float32)] * 2,
        ),
        out_shape=[wide, wide, wide],
        cost_estimate=pl.CostEstimate(
            flops=rows * rows * LANES * 4,
            bytes_accessed=rows * LANES * 24,
            transcendentals=rows * rows // 2,
        ),
        name="attend_back",
    )(
        row_lengths,
        queries,
        grads.reshape(dealt, groups, dealt, slot, LANES),
        stats,
        keys,
        values,
        keys_turned,
    )


def gelu_slope(values_in):
    scale = math.sqrt(2.0 / math.pi)
    bent = jnp.tanh(scale * (values_in + 0.044715 * values_in * values_in * values_in))
    return 0.5 * (1.0 + bent) + 0.5 * values_in * (1.0 - bent * bent) * scale * (
        1.0 + 3.0 * 0.044715 * values_in * values_in
    )


def schulz_chain(gram):
    precise = functools.partial(jnp.dot, precision=lax.Precision.HIGHEST)
    eye = jnp.eye(gram.shape[0], dtype=jnp.float32)
    chain = None
    for turn_id in range(SCHULZ_STEPS):
        turn = (
            SCHULZ_FIRST * eye + SCHULZ_SECOND * gram + SCHULZ_THIRD * precise(gram, gram)
        )
        chain = turn if chain is None else precise(turn, chain)
        if turn_id < SCHULZ_STEPS - 1:
            gram = precise(precise(turn, gram), turn)
    return chain


def gathered_weights(
    tokens,
    cotangent,
    placement,
    lengths,
    step_count,
    norm_gain,
    norm_bias,
    project_weight,
    project_bias,
    output_weight,
    output_bias,
    expand_weight,
    expand_bias,
    reduce_weight,
    reduce_bias,
    project_momentum,
    output_momentum,
    expand_momentum,
    reduce_momentum,
    norm_gain_first,
    norm_gain_second,
    norm_bias_first,
    norm_bias_second,
    project_bias_first,
    project_bias_second,
    output_bias_first,
    output_bias_second,
    expand_bias_first,
    expand_bias_second,
    reduce_bias_first,
    reduce_bias_second,
):
    fsdp_count = lax.axis_size("fsdp")
    ns_count = lax.axis_size("ns")
    shard_rows = tokens.shape[0]
    slot_rows = shard_rows // fsdp_count
    group_rows = shard_rows * ns_count
    pack_rows = group_rows * fsdp_count
    fsdp_at = lax.axis_index("fsdp")
    ns_at = lax.axis_index("ns")
    row_lengths = lengths[0]
    heads_here = project_bias.shape[0] // (3 * HEAD_DIM)
    head_cols = heads_here * HEAD_DIM
    scale_factor = HEAD_DIM ** (-0.5)
    within = placement % shard_rows
    dest_fsdp = placement // shard_rows // ns_count % fsdp_count
    slot_index = dest_fsdp * slot_rows + within - fsdp_at * slot_rows
    source_row = (
        jnp.zeros((shard_rows,), jnp.int32)
        .at[slot_index]
        .set(jnp.arange(shard_rows, dtype=jnp.int32))
    )
    dealt_tokens, dealt_cotangent = (
        lax.all_to_all(tokens[source_row], "fsdp", split_axis=0, concat_axis=0, tiled=True),
        lax.all_to_all(cotangent[source_row], "fsdp", split_axis=0, concat_axis=0, tiled=True),
    )
    token_rows = dealt_tokens.astype(jnp.float32)
    normed, norm_back = jax.vjp(layer_norm, token_rows, norm_gain, norm_bias)
    normed_low = normed.astype(jnp.bfloat16)
    normed_all, cotangent_all = (
        lax.all_gather(normed_low, "ns", axis=0, tiled=True),
        lax.all_gather(dealt_cotangent, "ns", axis=0, tiled=True),
    )
    project_low = project_weight.astype(jnp.bfloat16)
    output_low = output_weight.astype(jnp.bfloat16)
    expand_low = expand_weight.astype(jnp.bfloat16)
    reduce_low = reduce_weight.astype(jnp.bfloat16)
    project_full, output_full, expand_full, reduce_full = (
        lax.all_gather(project_low, "fsdp", axis=0, tiled=True),
        lax.all_gather(output_low, "fsdp", axis=1, tiled=True),
        lax.all_gather(expand_low, "fsdp", axis=0, tiled=True),
        lax.all_gather(reduce_low, "fsdp", axis=1, tiled=True),
    )
    group_first = fsdp_at * group_rows
    query_rows = group_first + jnp.arange(group_rows, dtype=jnp.int32)
    query_seq, query_starts = sequence_layout(row_lengths, query_rows)
    positions = query_rows - query_starts
    reach_first = query_starts[0]
    query_last = group_first + group_rows - 1
    cosine, sine = rope_tables(positions)
    joined = jnp.dot(normed_all, project_full, preferred_element_type=jnp.float32) + project_bias
    joined = joined.reshape(group_rows, heads_here, 3, HEAD_DIM)
    query_view = rotate(joined[:, :, 0], cosine, sine).astype(jnp.bfloat16)
    keys_here = (
        rotate(joined[:, :, 1], cosine, sine).astype(jnp.bfloat16).reshape(group_rows, head_cols)
    )
    values_here = joined[:, :, 2].astype(jnp.bfloat16).reshape(group_rows, head_cols)
    paired_here = jnp.stack([keys_here, values_here], axis=1)

    def wanted(key_first, key_count):
        return (key_first <= query_last) & (key_first + key_count - 1 >= reach_first)

    def piece_scores(key_piece, key_first):
        key_count = key_piece.shape[0]
        key_rows = key_first + jnp.arange(key_count, dtype=jnp.int32)
        key_seq = sequence_layout(row_lengths, key_rows)[0]
        scores = (
            jnp.einsum(
                "qhe,khe->hqk",
                query_view,
                key_piece.reshape(key_count, heads_here, HEAD_DIM),
                preferred_element_type=jnp.float32,
            )
            * scale_factor
        )
        allowed = (key_seq[None, :] == query_seq[:, None]) & (
            key_rows[None, :] <= query_rows[:, None]
        )
        return jnp.where(allowed[None], scores, NEG_LARGE)

    paired_group = lax.all_gather(paired_here, "fsdp", axis=0, tiled=True)
    paired_stack = paired_group.reshape(fsdp_count, group_rows, 2, head_cols)
    first_rows = jnp.arange(fsdp_count, dtype=jnp.int32) * group_rows

    def sweep(step_fn, initial):

        def scan_body(running, scan_item):
            return step_fn(running, scan_item[0][:, 0], scan_item[0][:, 1], scan_item[1])

        return lax.scan(scan_body, initial, (paired_stack, first_rows))

    def stats_step(running, key_piece, value_piece, key_first):

        def stats_compute(held_stats):
            row_top, row_sum = held_stats
            scores = piece_scores(key_piece, key_first)
            top_new = jnp.maximum(row_top, jnp.max(scores, axis=2))
            sum_new = row_sum * jnp.exp(row_top - top_new) + jnp.sum(
                jnp.exp(scores - top_new[:, :, None]), axis=2
            )
            return (top_new, sum_new)

        return (
            lax.cond(
                wanted(key_first, key_piece.shape[0]),
                stats_compute,
                lambda held_stats: held_stats,
                running,
            ),
            None,
        )

    initial_stats = (
        jnp.full((heads_here, group_rows), NEG_LARGE, jnp.float32),
        jnp.zeros((heads_here, group_rows), jnp.float32),
    )
    final_stats = sweep(stats_step, initial_stats)[0]
    log_total = final_stats[0] + jnp.log(final_stats[1])

    def output_step(running, key_piece, value_piece, key_first):
        key_count = key_piece.shape[0]

        def output_compute(accum):
            scores = piece_scores(key_piece, key_first)
            probs_low = jnp.exp(scores - log_total[:, :, None]).astype(jnp.bfloat16)
            return accum + jnp.einsum(
                "hqk,khe->qhe",
                probs_low,
                value_piece.reshape(key_count, heads_here, HEAD_DIM),
                preferred_element_type=jnp.float32,
            )

        return (
            lax.cond(wanted(key_first, key_count), output_compute, lambda accum: accum, running),
            None,
        )

    attended = sweep(output_step, jnp.zeros((group_rows, heads_here, HEAD_DIM), jnp.float32))[0]
    attended_low = attended.reshape(group_rows, head_cols).astype(jnp.bfloat16)
    hidden = jnp.dot(normed_all, expand_full, preferred_element_type=jnp.float32) + expand_bias
    activated, gelu_back = jax.vjp(gelu_tanh, hidden)
    activated_low = activated.astype(jnp.bfloat16)
    branch_sum = lax.psum_scatter(
        jnp.dot(attended_low, output_full, preferred_element_type=jnp.float32)
        + jnp.dot(activated_low, reduce_full, preferred_element_type=jnp.float32),
        "ns",
        scatter_dimension=0,
        tiled=True,
    )
    layer_rows = (token_rows + branch_sum + output_bias + reduce_bias).astype(jnp.bfloat16)
    back_project, back_output, back_expand, back_reduce = (
        lax.all_gather(project_low, "fsdp", axis=0, tiled=True),
        lax.all_gather(output_low, "fsdp", axis=1, tiled=True),
        lax.all_gather(expand_low, "fsdp", axis=0, tiled=True),
        lax.all_gather(reduce_low, "fsdp", axis=1, tiled=True),
    )
    d_attended = jnp.einsum(
        "td,hd->th", cotangent_all, back_output, preferred_element_type=jnp.float32
    ).astype(jnp.bfloat16)
    d_attended_view = d_attended.reshape(group_rows, heads_here, HEAD_DIM)
    d_activated = jnp.einsum(
        "td,fd->tf", cotangent_all, back_reduce, preferred_element_type=jnp.float32
    )
    d_hidden = gelu_back(d_activated)[0].astype(jnp.bfloat16)

    def delta_step(running, key_piece, value_piece, key_first):
        key_count = key_piece.shape[0]

        def delta_compute(accum):
            scores = piece_scores(key_piece, key_first)
            probs = jnp.exp(scores - log_total[:, :, None])
            d_probs = jnp.einsum(
                "qhe,khe->hqk",
                d_attended_view,
                value_piece.reshape(key_count, heads_here, HEAD_DIM),
                preferred_element_type=jnp.float32,
            )
            return accum + jnp.sum(probs * d_probs, axis=2)

        return (
            lax.cond(wanted(key_first, key_count), delta_compute, lambda accum: accum, running),
            None,
        )

    delta = sweep(delta_step, jnp.zeros((heads_here, group_rows), jnp.float32))[0]

    def grads_step(running, key_piece, value_piece, key_first):
        key_count = key_piece.shape[0]

        def grads_compute(d_queries):
            keys_view = key_piece.reshape(key_count, heads_here, HEAD_DIM)
            values_view = value_piece.reshape(key_count, heads_here, HEAD_DIM)
            scores = piece_scores(key_piece, key_first)
            probs = jnp.exp(scores - log_total[:, :, None])
            d_probs = jnp.einsum(
                "qhe,khe->hqk", d_attended_view, values_view, preferred_element_type=jnp.float32
            )
            d_scores = (probs * (d_probs - delta[:, :, None])).astype(jnp.bfloat16)
            d_queries = (
                d_queries
                + jnp.einsum(
                    "hqk,khe->qhe", d_scores, keys_view, preferred_element_type=jnp.float32
                )
                * scale_factor
            )
            d_keys = (
                jnp.einsum("hqk,qhe->khe", d_scores, query_view, preferred_element_type=jnp.float32)
                * scale_factor
            )
            d_values = jnp.einsum(
                "hqk,qhe->khe",
                probs.astype(jnp.bfloat16),
                d_attended_view,
                preferred_element_type=jnp.float32,
            )
            return (
                d_queries,
                jnp.stack(
                    [d_keys.reshape(key_count, head_cols), d_values.reshape(key_count, head_cols)],
                    axis=1,
                ),
            )

        def skipped(d_queries):
            return (d_queries, jnp.zeros((key_count, 2, head_cols), jnp.float32))

        return lax.cond(wanted(key_first, key_count), grads_compute, skipped, running)

    d_queries, key_extras = sweep(
        grads_step, jnp.zeros((group_rows, heads_here, HEAD_DIM), jnp.float32)
    )
    key_sums = lax.psum_scatter(
        key_extras.reshape(pack_rows, 2, head_cols), "fsdp", scatter_dimension=0, tiled=True
    )
    d_keys_own = key_sums[:, 0].reshape(group_rows, heads_here, HEAD_DIM)
    d_values_own = key_sums[:, 1].reshape(group_rows, heads_here, HEAD_DIM)
    d_joined = jnp.stack(
        [rotate(d_queries, cosine, -sine), rotate(d_keys_own, cosine, -sine), d_values_own], axis=2
    )
    d_joined = d_joined.reshape(group_rows, 3 * head_cols).astype(jnp.bfloat16)
    d_normed = lax.psum_scatter(
        jnp.einsum("tc,dc->td", d_joined, back_project, preferred_element_type=jnp.float32)
        + jnp.einsum("tf,df->td", d_hidden, back_expand, preferred_element_type=jnp.float32),
        "ns",
        scatter_dimension=0,
        tiled=True,
    )
    d_tokens_norm, gain_term, shift_term = norm_back(d_normed)
    input_rows = (dealt_cotangent.astype(jnp.float32) + d_tokens_norm).astype(jnp.bfloat16)
    back_layer, back_input = (
        lax.all_to_all(layer_rows, "fsdp", split_axis=0, concat_axis=0, tiled=True),
        lax.all_to_all(input_rows, "fsdp", split_axis=0, concat_axis=0, tiled=True),
    )
    layer_output = back_layer[slot_index]
    input_grad = back_input[slot_index]
    project_term = jnp.einsum("td,tc->dc", normed_all, d_joined, preferred_element_type=jnp.float32)
    output_term = jnp.einsum(
        "th,td->hd", attended_low, cotangent_all, preferred_element_type=jnp.float32
    )
    expand_term = jnp.einsum("td,tf->df", normed_all, d_hidden, preferred_element_type=jnp.float32)
    reduce_term = jnp.einsum(
        "tf,td->fd", activated_low, cotangent_all, preferred_element_type=jnp.float32
    )
    shards = (
        lax.psum_scatter(project_term, "fsdp", scatter_dimension=0, tiled=True),
        lax.psum_scatter(output_term, "fsdp", scatter_dimension=1, tiled=True),
        lax.psum_scatter(expand_term, "fsdp", scatter_dimension=0, tiled=True),
        lax.psum_scatter(reduce_term, "fsdp", scatter_dimension=1, tiled=True),
    )
    project_grad, output_grad, expand_grad, reduce_grad = lax.psum(
        (shards[0], shards[1], shards[2], shards[3]), "rep"
    )
    project_bias_width = project_bias.shape[0]
    expand_bias_width = expand_bias.shape[0]
    project_bias_part = lax.dynamic_update_slice(
        jnp.zeros((project_bias_width * ns_count,), jnp.float32),
        jnp.sum(d_joined, axis=0, dtype=jnp.float32),
        (ns_at * project_bias_width,),
    )
    expand_bias_part = lax.dynamic_update_slice(
        jnp.zeros((expand_bias_width * ns_count,), jnp.float32),
        jnp.sum(d_hidden, axis=0, dtype=jnp.float32),
        (ns_at * expand_bias_width,),
    )
    cotangent_sum = jnp.sum(dealt_cotangent, axis=0, dtype=jnp.float32)
    gain_grad, shift_grad, cotangent_total, project_bias_all, expand_bias_all = lax.psum(
        (gain_term, shift_term, cotangent_sum, project_bias_part, expand_bias_part),
        ("rep", "fsdp", "ns"),
    )
    project_bias_grad = lax.dynamic_slice_in_dim(
        project_bias_all, ns_at * project_bias_width, project_bias_width
    )
    expand_bias_grad = lax.dynamic_slice_in_dim(
        expand_bias_all, ns_at * expand_bias_width, expand_bias_width
    )
    project_mom = MUON_DECAY * project_momentum + project_grad
    output_mom = MUON_DECAY * output_momentum + output_grad
    expand_mom = MUON_DECAY * expand_momentum + expand_grad
    reduce_mom = MUON_DECAY * reduce_momentum + reduce_grad
    current = (project_mom, output_mom.T, expand_mom, reduce_mom.T)
    for turn_id in range(SCHULZ_STEPS):
        grams = lax.psum(
            (
                local_gram(current[0]),
                local_gram(current[1]),
                local_gram(current[2]),
                local_gram(current[3]),
            ),
            "ns",
        )
        if turn_id == 0:
            factors = [lax.rsqrt(jnp.trace(gram_sum) + SCHULZ_EPSILON) for gram_sum in grams]
            current = tuple(
                (block_part * factor_now for block_part, factor_now in zip(current, factors))
            )
            grams = tuple(
                (
                    gram_sum * (factor_now * factor_now)
                    for gram_sum, factor_now in zip(grams, factors)
                )
            )
        current = tuple(
            (schulz_turn(block_part, gram_sum) for block_part, gram_sum in zip(current, grams))
        )
    project_new = muon_weight(project_weight, current[0], 3 * D)
    output_new = muon_weight(output_weight, current[1].T, D)
    expand_new = muon_weight(expand_weight, current[2], FF)
    reduce_new = muon_weight(reduce_weight, current[3].T, FF)
    gain_new, gain_one, gain_two = adam_update(
        norm_gain, norm_gain_first, norm_gain_second, gain_grad, step_count
    )
    shift_new, shift_one, shift_two = adam_update(
        norm_bias, norm_bias_first, norm_bias_second, shift_grad, step_count
    )
    pbias_new, pbias_one, pbias_two = adam_update(
        project_bias, project_bias_first, project_bias_second, project_bias_grad, step_count
    )
    obias_new, obias_one, obias_two = adam_update(
        output_bias, output_bias_first, output_bias_second, cotangent_total, step_count
    )
    ebias_new, ebias_one, ebias_two = adam_update(
        expand_bias, expand_bias_first, expand_bias_second, expand_bias_grad, step_count
    )
    rbias_new, rbias_one, rbias_two = adam_update(
        reduce_bias, reduce_bias_first, reduce_bias_second, cotangent_total, step_count
    )
    return (
        layer_output,
        input_grad,
        gain_grad,
        shift_grad,
        project_grad,
        project_bias_grad,
        output_grad,
        cotangent_total,
        expand_grad,
        expand_bias_grad,
        reduce_grad,
        cotangent_total,
        gain_new,
        shift_new,
        project_new,
        pbias_new,
        output_new,
        obias_new,
        expand_new,
        ebias_new,
        reduce_new,
        rbias_new,
        project_new.astype(jnp.bfloat16),
        output_new.astype(jnp.bfloat16),
        expand_new.astype(jnp.bfloat16),
        reduce_new.astype(jnp.bfloat16),
        project_mom,
        output_mom,
        expand_mom,
        reduce_mom,
        gain_one,
        gain_two,
        shift_one,
        shift_two,
        pbias_one,
        pbias_two,
        obias_one,
        obias_two,
        ebias_one,
        ebias_two,
        rbias_one,
        rbias_two,
    )


def per_device(axis_sizes, *arguments):
    heads = arguments[8].shape[0] // (3 * HEAD_DIM)
    shard_rows = arguments[0].shape[0]
    dealt = axis_sizes["fsdp"]
    fits = heads * HEAD_DIM == dealt * LANES and shard_rows == BLOCK and BLOCK % (8 * dealt) == 0
    return (split_heads if fits else gathered_weights)(*arguments)


def split_heads(
    tokens,
    cotangent,
    placement,
    lengths,
    step_count,
    norm_gain,
    norm_bias,
    project_weight,
    project_bias,
    output_weight,
    output_bias,
    expand_weight,
    expand_bias,
    reduce_weight,
    reduce_bias,
    project_momentum,
    output_momentum,
    expand_momentum,
    reduce_momentum,
    norm_gain_first,
    norm_gain_second,
    norm_bias_first,
    norm_bias_second,
    project_bias_first,
    project_bias_second,
    output_bias_first,
    output_bias_second,
    expand_bias_first,
    expand_bias_second,
    reduce_bias_first,
    reduce_bias_second,
):
    dealt = lax.axis_size("fsdp")
    groups = lax.axis_size("ns")
    shard_rows = tokens.shape[0]
    slot = shard_rows // dealt
    pack_rows = shard_rows * dealt * groups
    fsdp_at = lax.axis_index("fsdp")
    ns_at = lax.axis_index("ns")
    row_lengths = lengths[0]
    low = jnp.bfloat16

    within = placement % shard_rows
    dest = placement // shard_rows // groups % dealt
    slot_index = dest * slot + within - fsdp_at * slot
    slots = jnp.arange(shard_rows, dtype=jnp.int32)
    deal = (slot_index[None, :] == slots[:, None]).astype(low)
    sorted_tokens = jnp.dot(deal, tokens, preferred_element_type=jnp.float32)
    sorted_cotangent = jnp.dot(deal, cotangent, preferred_element_type=jnp.float32).astype(low)
    normed, norm_back = jax.vjp(layer_norm, sorted_tokens, norm_gain, norm_bias)
    normed_all = lax.all_gather(normed.astype(low), ("fsdp", "ns"), axis=0, tiled=True)

    def exchange(pieces):
        return lax.all_to_all(pieces, "fsdp", split_axis=0, concat_axis=0, tiled=True)

    col = jnp.arange(3 * LANES, dtype=jnp.int32)
    dest_col = (
        col % (3 * HEAD_DIM) // HEAD_DIM * LANES
        + col // (3 * HEAD_DIM) * HEAD_DIM
        + col % HEAD_DIM
    )
    shuffle = (dest_col[:, None] == col[None, :]).astype(low)
    width = project_weight.shape[0]
    ff_here = expand_bias.shape[0] // dealt
    project_pieces = jnp.einsum(
        "rfc,cd->frd",
        project_weight.astype(low).reshape(width, dealt, 3 * LANES),
        shuffle,
        preferred_element_type=low,
    )
    project_full = exchange(project_pieces).reshape(dealt * width, 3 * LANES)
    expand_pieces = expand_weight.astype(low).reshape(width, dealt, ff_here).transpose(1, 0, 2)
    expand_full = exchange(expand_pieces).reshape(dealt * width, ff_here)
    output_pieces = output_weight.astype(low).reshape(dealt, LANES, width)
    output_full = exchange(output_pieces).transpose(1, 0, 2).reshape(LANES, dealt * width)
    reduce_pieces = reduce_weight.astype(low).reshape(dealt, ff_here, width)
    reduce_full = exchange(reduce_pieces).transpose(1, 0, 2).reshape(ff_here, dealt * width)

    normed_all, expand_full, output_full, reduce_full = lax.optimization_barrier(
        (normed_all, expand_full, output_full, reduce_full)
    )
    pack_ids = jnp.arange(pack_rows, dtype=jnp.int32)
    positions = pack_ids - sequence_layout(row_lengths, pack_ids)[1]
    cosine_half, sine_half = rope_tables(positions)
    still = jnp.zeros((pack_rows, HEAD_DIM - ROT), jnp.float32)
    head_cosine = jnp.concatenate([cosine_half, cosine_half, still + 1.0], axis=1)
    head_sine = jnp.concatenate([-sine_half, sine_half, still], axis=1)
    cosine = jnp.concatenate([head_cosine, head_cosine], axis=1)
    sine = jnp.concatenate([head_sine, head_sine], axis=1)

    project_bias_here = lax.dynamic_slice_in_dim(project_bias, fsdp_at * 3 * LANES, 3 * LANES)
    project_bias_here = (
        project_bias_here.reshape(-1, 3, HEAD_DIM).transpose(1, 0, 2).reshape(3 * LANES)
    )
    expand_bias_here = lax.dynamic_slice_in_dim(expand_bias, fsdp_at * ff_here, ff_here)
    joined = (
        jnp.dot(normed_all, project_full, preferred_element_type=jnp.float32) + project_bias_here
    )
    later_cotangent, joined = lax.optimization_barrier((sorted_cotangent, joined))
    cotangent_all = lax.all_gather(later_cotangent, ("fsdp", "ns"), axis=0, tiled=True)
    queries, keys, values, keys_turned, values_turned = rope(joined, cosine, sine, dealt, groups)
    attended_low, stats = attend(row_lengths, queries, keys, values_turned, dealt, groups)
    hidden = jnp.dot(normed_all, expand_full, preferred_element_type=jnp.float32) + expand_bias_here
    activated_low = gelu_tanh(hidden).astype(low)
    branch = jnp.dot(attended_low, output_full, preferred_element_type=jnp.float32) + jnp.dot(
        activated_low, reduce_full, preferred_element_type=jnp.float32
    )
    branch_low, cotangent_all = lax.optimization_barrier((branch.astype(low), cotangent_all))
    branch_sum = lax.psum_scatter(branch_low, ("fsdp", "ns"), scatter_dimension=0, tiled=True)

    d_attended = dot_nt(cotangent_all, output_full).astype(low)
    d_hidden = (gelu_slope(hidden) * dot_nt(cotangent_all, reduce_full)).astype(low)
    d_queries, d_keys, d_values = attend_back(
        row_lengths, queries, d_attended, stats, keys, values, keys_turned, dealt, groups
    )
    d_joined, d_joined_sum = unrope(d_queries, d_keys, d_values, cosine, sine, dealt, groups)
    d_normed_part = dot_nt(d_joined, project_full) + dot_nt(d_hidden, expand_full)
    d_normed_low, normed_all, branch_sum = lax.optimization_barrier(
        (d_normed_part.astype(low), normed_all, branch_sum)
    )
    d_normed = lax.psum_scatter(d_normed_low, ("fsdp", "ns"), scatter_dimension=0, tiled=True)
    branch_sum = branch_sum.astype(jnp.float32)
    layer_rows = (sorted_tokens + branch_sum + output_bias + reduce_bias).astype(low)
    def outer(left, right):
        return lax.dot_general(
            left, right, (((0,), (0,)), ((), ())), preferred_element_type=jnp.float32
        ).astype(low)

    def both_packs(shard):
        twin = lax.ppermute(shard, "rep", [(0, 1), (1, 0)]) if lax.axis_size("rep") == 2 else None
        if twin is None:
            return lax.psum(shard.astype(jnp.float32), "rep")
        return shard.astype(jnp.float32) + twin.astype(jnp.float32)

    reduce_term = outer(activated_low, cotangent_all).reshape(ff_here, dealt, width)
    reduce_grad = both_packs(
        exchange(reduce_term.transpose(1, 0, 2)).reshape(dealt * ff_here, width)
    )
    output_term = outer(attended_low, cotangent_all).reshape(LANES, dealt, width)
    output_grad = both_packs(
        exchange(output_term.transpose(1, 0, 2)).reshape(dealt * LANES, width)
    )
    expand_term = outer(normed_all, d_hidden).reshape(dealt, width, ff_here)
    expand_grad = both_packs(
        exchange(expand_term).transpose(1, 0, 2).reshape(width, dealt * ff_here)
    )
    project_term = jnp.einsum(
        "frd,cd->frc",
        outer(normed_all, d_joined).reshape(dealt, width, 3 * LANES),
        shuffle,
        preferred_element_type=low,
    )
    project_grad = both_packs(
        exchange(project_term).transpose(1, 0, 2).reshape(width, dealt * 3 * LANES)
    )

    project_mom = MUON_DECAY * project_momentum + project_grad
    output_mom = MUON_DECAY * output_momentum + output_grad
    expand_mom = MUON_DECAY * expand_momentum + expand_grad
    reduce_mom = MUON_DECAY * reduce_momentum + reduce_grad
    precise = functools.partial(lax.dot_general, precision=lax.Precision.HIGHEST)
    by_row = (((1,), (1,)), ((), ()))
    by_col = (((0,), (0,)), ((), ()))
    grams = jnp.stack(
        [
            precise(project_mom, project_mom, by_row),
            precise(output_mom, output_mom, by_col),
            precise(expand_mom, expand_mom, by_row),
            precise(reduce_mom, reduce_mom, by_col),
        ]
    )
    grams, d_normed = lax.optimization_barrier((grams, d_normed))
    d_tokens_norm, gain_term, shift_term = norm_back(d_normed.astype(jnp.float32))
    input_rows = (sorted_cotangent.astype(jnp.float32) + d_tokens_norm).astype(low)

    def undeal(rows):
        return lax.dot_general(
            deal, rows, (((0,), (0,)), ((), ())), preferred_element_type=jnp.float32
        ).astype(low)

    layer_output = undeal(layer_rows)
    input_grad = undeal(input_rows)

    part_at = ns_at * dealt + fsdp_at
    project_bias_width = project_bias.shape[0]
    expand_bias_width = expand_bias.shape[0]
    project_bias_part = lax.dynamic_update_slice(
        jnp.zeros((project_bias_width * groups,), jnp.float32),
        d_joined_sum.reshape(3, -1, HEAD_DIM).transpose(1, 0, 2).reshape(3 * LANES),
        (part_at * 3 * LANES,),
    )
    expand_bias_part = lax.dynamic_update_slice(
        jnp.zeros((expand_bias_width * groups,), jnp.float32),
        jnp.sum(d_hidden, axis=0, dtype=jnp.float32),
        (part_at * ff_here,),
    )
    cotangent_sum = jnp.sum(sorted_cotangent, axis=0, dtype=jnp.float32)
    gain_grad, shift_grad, cotangent_total, project_bias_all, expand_bias_all = lax.psum(
        (gain_term, shift_term, cotangent_sum, project_bias_part, expand_bias_part),
        ("rep", "fsdp", "ns"),
    )
    project_bias_grad = lax.dynamic_slice_in_dim(
        project_bias_all, ns_at * project_bias_width, project_bias_width
    )
    expand_bias_grad = lax.dynamic_slice_in_dim(
        expand_bias_all, ns_at * expand_bias_width, expand_bias_width
    )

    gram = lax.psum_scatter(grams, "ns", scatter_dimension=0, tiled=True)[0]
    factor = lax.rsqrt(jnp.trace(gram) + SCHULZ_EPSILON)
    chain = schulz_chain(gram * (factor * factor)) * factor
    chains = lax.all_gather(chain, "ns", axis=0)
    left = (((1,), (0,)), ((), ()))
    right = (((1,), (1,)), ((), ()))
    project_new = muon_weight(project_weight, precise(chains[0], project_mom, left), 3 * D)
    output_new = muon_weight(output_weight, precise(output_mom, chains[1], right), D)
    expand_new = muon_weight(expand_weight, precise(chains[2], expand_mom, left), FF)
    reduce_new = muon_weight(reduce_weight, precise(reduce_mom, chains[3], right), FF)

    gain_new, gain_one, gain_two = adam_update(
        norm_gain, norm_gain_first, norm_gain_second, gain_grad, step_count
    )
    shift_new, shift_one, shift_two = adam_update(
        norm_bias, norm_bias_first, norm_bias_second, shift_grad, step_count
    )
    pbias_new, pbias_one, pbias_two = adam_update(
        project_bias, project_bias_first, project_bias_second, project_bias_grad, step_count
    )
    obias_new, obias_one, obias_two = adam_update(
        output_bias, output_bias_first, output_bias_second, cotangent_total, step_count
    )
    ebias_new, ebias_one, ebias_two = adam_update(
        expand_bias, expand_bias_first, expand_bias_second, expand_bias_grad, step_count
    )
    rbias_new, rbias_one, rbias_two = adam_update(
        reduce_bias, reduce_bias_first, reduce_bias_second, cotangent_total, step_count
    )
    return (
        layer_output,
        input_grad,
        gain_grad,
        shift_grad,
        project_grad,
        project_bias_grad,
        output_grad,
        cotangent_total,
        expand_grad,
        expand_bias_grad,
        reduce_grad,
        cotangent_total,
        gain_new,
        shift_new,
        project_new,
        pbias_new,
        output_new,
        obias_new,
        expand_new,
        ebias_new,
        reduce_new,
        rbias_new,
        project_new.astype(jnp.bfloat16),
        output_new.astype(jnp.bfloat16),
        expand_new.astype(jnp.bfloat16),
        reduce_new.astype(jnp.bfloat16),
        project_mom,
        output_mom,
        expand_mom,
        reduce_mom,
        gain_one,
        gain_two,
        shift_one,
        shift_two,
        pbias_one,
        pbias_two,
        obias_one,
        obias_two,
        ebias_one,
        ebias_two,
        rbias_one,
        rbias_two,
    )


def solution(mesh):
    return jax.shard_map(
        functools.partial(per_device, dict(mesh.shape)),
        mesh=mesh,
        in_specs=(
            P(("rep", "fsdp", "ns"), None),
            P(("rep", "fsdp", "ns"), None),
            P(("rep", "fsdp", "ns")),
            P("rep", None),
            P(),
            P(),
            P(),
            P("fsdp", "ns"),
            P("ns"),
            P("ns", "fsdp"),
            P(),
            P("fsdp", "ns"),
            P("ns"),
            P("ns", "fsdp"),
            P(),
            P("fsdp", "ns"),
            P("ns", "fsdp"),
            P("fsdp", "ns"),
            P("ns", "fsdp"),
            P(),
            P(),
            P(),
            P(),
            P("ns"),
            P("ns"),
            P(),
            P(),
            P("ns"),
            P("ns"),
            P(),
            P(),
        ),
        out_specs=(
            P(("rep", "fsdp", "ns"), None),
            P(("rep", "fsdp", "ns"), None),
            P(),
            P(),
            P("fsdp", "ns"),
            P("ns"),
            P("ns", "fsdp"),
            P(),
            P("fsdp", "ns"),
            P("ns"),
            P("ns", "fsdp"),
            P(),
            P(),
            P(),
            P("fsdp", "ns"),
            P("ns"),
            P("ns", "fsdp"),
            P(),
            P("fsdp", "ns"),
            P("ns"),
            P("ns", "fsdp"),
            P(),
            P("fsdp", "ns"),
            P("ns", "fsdp"),
            P("fsdp", "ns"),
            P("ns", "fsdp"),
            P("fsdp", "ns"),
            P("ns", "fsdp"),
            P("fsdp", "ns"),
            P("ns", "fsdp"),
            P(),
            P(),
            P(),
            P(),
            P("ns"),
            P("ns"),
            P(),
            P(),
            P("ns"),
            P("ns"),
            P(),
            P(),
        ),
        check_vma=False,
    )
```
